128 devices in a mesh: dp: 16 (over x_lo, y, core), layer: 8 (over x_hi, z).
Axes of the slice: x: 4 (x_hi: 2, x_lo: 2; x = x_hi * 2 + x_lo), y: 4, z: 4, core: 2. Of those that a mesh axis runs over, the one named last changes fastest.
Arguments:
- activations: bfloat16 [4096, 8, 7168], P('dp', 'layer'), may hold values from -200 to 200
- labels: int32 [4096], P('dp'), may hold values from 0 to 511
- weights: float32 [7168, 8, 512], P('dp', 'layer'), may hold values from -0.0625 to 0.0625
- first_moment: float32 [7168, 8, 512], P('dp', 'layer'), may hold values from -0.00036621094 to 0.00036621094
- second_moment: float32 [7168, 8, 512], P('dp', 'layer'), may hold values from 2.1287373e-12 to 2.1287373e-11
Outputs:
- new_weights: float32 [7168, 8, 512], P('dp', 'layer')
- new_first: float32 [7168, 8, 512], P('dp', 'layer')
- new_second: float32 [7168, 8, 512], P('dp', 'layer')
- loss: float32 [], replicated
The draws below stay inside these ranges and needn't reach their ends.
All inputs are finite; a program needn't handle non-finite values.
Results may differ from the reference program's by a relative error of at most 0.0014.
Values may be sent and summed in bfloat16 or wider, within the bound.
A program may use at most 128 MiB of HBM per device.

```python
import math
import jax
import jax.numpy as jnp
import numpy as np
from jax import lax

D = 7168
C = 512
STEP = 10
TOKENS = 4096
LAYERS = 8


def draw_activations(key, part):
    key_base = jax.random.fold_in(key, 11)
    key_rough = jax.random.fold_in(key, 12)
    key_centre = jax.random.fold_in(key, 15)
    tok_pos = jnp.arange(TOKENS, dtype=jnp.float32) / max(TOKENS - 1, 1)
    lay_pos = jnp.arange(LAYERS, dtype=jnp.float32) / max(LAYERS - 1, 1)
    trend = (1.0 + 2.0 * tok_pos)[:, None] * (1.0 + 2.0 * lay_pos)[None, :]
    rough = jnp.exp(jax.random.uniform(key_rough, (TOKENS, LAYERS), jnp.float32) * math.log(10.0)) / 10.0
    scale = trend * rough
    centre = jnp.clip(jax.random.normal(key_centre, (LAYERS, D), jnp.float32), -4.0, 4.0)
    base = jax.random.normal(key_base, (TOKENS, LAYERS, D), jnp.float32)
    values = jnp.clip(base * scale[:, :, None] + centre[None, :, :], -200.0, 200.0)
    return values.astype(jnp.bfloat16)


def touch_ends(drawn, key, smallest, largest):
    longest = drawn.shape.index(max(drawn.shape))
    spots = []
    for shift in (0, 1):
        where = [jax.random.randint(jax.random.fold_in(key, axis), (), 0, length) for axis, length in enumerate(drawn.shape)]
        where[longest] = (where[longest] + shift) % drawn.shape[longest]
        spots.append(tuple(where))
    return drawn.at[spots[0]].set(smallest).at[spots[1]].set(largest)


def shard_levels(stream_key, shape, cuts, low, high):
    def one(position, parts):
        draws = jax.random.uniform(jax.random.fold_in(jax.random.fold_in(stream_key, 6), position), (parts,), jnp.float32, low / len(cuts), high / len(cuts))
        return jnp.repeat(jnp.exp(draws), shape[position] // parts).reshape((-1,) + (1,) * (len(shape) - position - 1))

    gain = one(*cuts[0])
    for cut in cuts[1:]:
        gain = gain * one(*cut)
    return gain


def cumulative_ranks(amount, lean):
    portions = [(1 << 20) // math.isqrt(standing ** lean) + 1 for standing in range(1, amount + 1)]
    width = 1 + sum(portions) // (1 << 30)
    return np.cumsum(np.array([max(1, weight // width) for weight in portions]))


def skewed_ids(key, dims, count, lean):
    table = cumulative_ranks(count, lean)
    lot = jax.random.randint(jax.random.fold_in(key, 1), dims, 0, int(table[count - 1]))
    standing = jnp.searchsorted(jnp.asarray(table, jnp.int32), lot, side="right")
    return jax.random.permutation(jax.random.fold_in(key, 2), count)[standing].astype(jnp.int32)


def noise(stream_key, shape, scale, bound, cuts=(), held_as=jnp.bfloat16):
    array = jax.random.normal(stream_key, shape, jnp.float32) * scale
    if len(cuts) > 0:
        array = shard_levels(stream_key, shape, cuts, -0.22, 0.18) * array
    return jnp.clip(array, min=-bound, max=bound).astype(held_as)


def setup_inputs(seed: int = 0) -> dict:
    seeds = jax.random.split(jax.random.key(seed), 6)
    activations = draw_activations(jax.random.fold_in(seeds[5], 71), 0)
    labels = touch_ends(skewed_ids(seeds[1], (TOKENS,), C, 2), jax.random.fold_in(seeds[1], 3), 0, C - 1).astype(jnp.int32)
    weights = noise(seeds[2], (D, LAYERS, C), D ** -0.5, 0.0625, ((0, 16), (1, 8)), jnp.float32)
    first_moment = noise(seeds[3], (D, LAYERS, C), (0.125 / (D * LAYERS * C) ** 0.5), 0.00036621094, ((0, 16), (1, 8)), jnp.float32)
    second_moment = jnp.clip(jnp.exp(math.log(2.1287372906075852e-11) - 2.3025851 * jax.random.uniform(seeds[4], (D, LAYERS, C), jnp.float32) ** shard_levels(seeds[4], (D, LAYERS, C), ((0, 16), (1, 8)), -0.2, 0.2)), 2.1287372906075852e-12, 2.1287372906075852e-11)
    return dict(activations=activations, labels=labels, weights=weights, first_moment=first_moment, second_moment=second_moment)


def reference(activations, labels, weights, first_moment, second_moment):
    low_weights = weights.astype(jnp.bfloat16)
    classes = jnp.arange(C, dtype=jnp.int32)
    onehot = (labels[:, None] == classes[None, :]).astype(jnp.float32)
    total = jnp.zeros((), jnp.float32)
    columns = []
    for layer in range(LAYERS):
        feats = activations[:, layer, :]
        logits = jnp.dot(feats, low_weights[:, layer, :], preferred_element_type=jnp.float32)
        top = lax.optimization_barrier(jnp.max(logits, axis=1, keepdims=True))
        exps = jnp.exp(logits - top)
        denom = lax.optimization_barrier(jnp.sum(exps, axis=1, keepdims=True))
        picked = lax.optimization_barrier(jnp.sum(logits * onehot, axis=1))
        total = total + jnp.sum(top[:, 0] + jnp.log(denom[:, 0]) - picked)
        probs = exps / denom
        slope = ((probs - onehot) / TOKENS).astype(jnp.bfloat16)
        columns.append(jnp.dot(feats.T, slope, preferred_element_type=jnp.float32))
    grad = jnp.stack(columns, axis=1)
    loss = total / (TOKENS * LAYERS)
    square = jnp.sum(grad * grad)
    factor = jnp.minimum(1.0, 0.25 / jnp.sqrt(square + 1e-12))
    clipped = factor * grad
    new_first = 0.9 * first_moment + 0.1 * clipped
    new_second = 0.999 * second_moment + 0.001 * clipped * clipped
    new_weights = weights - 0.001 * (new_first / (1.0 - 0.9 ** STEP)) / (jnp.sqrt(new_second / (1.0 - 0.999 ** STEP)) + 1e-08)
    return (new_weights, new_first, new_second, loss)
```

```python
import jax
import jax.numpy as jnp
from jax import lax
from jax.experimental import pallas as pl
from jax.experimental.pallas import tpu as pltpu
from jax.sharding import PartitionSpec as P

STEP = 10
BF16 = jnp.bfloat16
F32 = jnp.float32
MESH = pl.DeviceIdType.MESH


def kernel(
    tokens,
    a_hbm,
    labels_ref,
    w_hbm,
    grad_ref,
    sums_ref,
    a_v,
    w32,
    wbuf,
    arx,
    slopes,
    acc,
    part,
    dbuf,
    xsend,
    xrecv,
    slots1,
    slots2,
    ld_sem,
    ws_sem,
    wr_sem,
    ds_sem,
    dr_sem,
    as_sem,
    ar_sem,
    ss_sem,
    sr_sem,
    es_sem,
    er_sem,
    xs_sem,
    xr_sem,
    p1s,
    p1r,
    p2s,
    p2r,
):
    tok = a_v.shape[0]
    width = wbuf.shape[1]
    rows = wbuf.shape[0] // 16
    half = rows // 2
    chip = 2 * rows
    d = lax.axis_index("dp")
    lay = lax.axis_index("layer")
    x = d // 8
    y = (d // 2) % 4
    c = d % 2

    def dp_of(dx, dy, dc=0):
        return ((x + dx) % 2) * 8 + ((y + dy) % 4) * 2 + (c + dc) % 2

    load_a = pltpu.make_async_copy(a_hbm, a_v, ld_sem.at[0])
    load_w = pltpu.make_async_copy(w_hbm, w32, ld_sem.at[1])
    load_w.start()
    load_a.start()

    barrier = pltpu.get_barrier_semaphore()
    near = [(1, 0, 0), (0, 1, 0), (0, 3, 0), (0, 2, 0), (0, 0, 1)]
    for dx, dy, dc in near:
        pl.semaphore_signal(
            barrier, inc=1, device_id={"dp": dp_of(dx, dy, dc)}, device_id_type=MESH
        )
    for k in range(1, 8):
        pl.semaphore_signal(
            barrier, inc=1, device_id={"layer": (lay + k) % 8}, device_id_type=MESH
        )

    load_w.wait()
    own = pl.multiple_of(d * rows, 64)

    def convert(g, carry):
        for j in range(4):
            v = w32[pl.ds(g * 64 + j, 16, stride=4), :]
            wbuf[pl.ds(pl.multiple_of(own + g * 16, 16), 16), j * 128 : (j + 1) * 128] = v.astype(BF16)
        return carry

    lax.fori_loop(0, rows // 16, convert, 0)
    pl.semaphore_wait(barrier, len(near) + 7)

    sent = []

    def send(src, dst, ssem, rsem, dp):
        cp = pltpu.make_async_remote_copy(
            src_ref=src, dst_ref=dst, send_sem=ssem, recv_sem=rsem,
            device_id={"dp": dp}, device_id_type=MESH,
        )
        cp.start()
        sent.append(cp)
        return cp

    def w_rows(dx, dy, dc, h):
        start = pl.multiple_of(dp_of(dx, dy, dc) * rows + h * half, 32)
        return wbuf.at[pl.ds(start, half), :]

    wcount = [0]

    def w_send(dx, dy, h, tx, ty):
        ref = w_rows(dx, dy, 0, h)
        k = ((dx - tx) % 2) * 4 + (dy - ty) % 4
        i = wcount[0]
        wcount[0] += 1
        send(ref, ref, ws_sem.at[i], wr_sem.at[k, h], dp_of(tx, ty))

    def w_pass(dx, dy, h):
        ref = w_rows(dx, dy, 0, h)
        k = dx * 4 + dy
        send(ref, ref, ds_sem.at[k, h], dr_sem.at[k, h], dp_of(0, 0, 1))

    def w_wait(dx, dy, h):
        ref = w_rows(dx, dy, 0, h)
        pltpu.make_async_remote_copy(
            src_ref=ref, dst_ref=ref, send_sem=ws_sem.at[0], recv_sem=wr_sem.at[dx * 4 + dy, h],
            device_id={"dp": dp_of(0, 0, 1)}, device_id_type=MESH,
        ).wait_recv()

    def d_wait(dx, dy, h):
        ref = w_rows(dx, dy, 1, h)
        pltpu.make_async_remote_copy(
            src_ref=ref, dst_ref=ref, send_sem=ws_sem.at[0], recv_sem=dr_sem.at[dx * 4 + dy, h],
            device_id={"dp": dp_of(0, 0, 1)}, device_id_type=MESH,
        ).wait_recv()

    def a_cols(dx, dy):
        return pl.multiple_of((((x + dx) % 2) * 4 + (y + dy) % 4) * chip, 128)

    def a_send(e, dx, dy):
        send(
            a_hbm.at[:, pl.ds(a_cols(dx, dy), chip)], arx.at[dy - 1, e],
            as_sem.at[dy - 1, e], ar_sem.at[dy - 1, e], dp_of(0, dy),
        )

    def a_wait(e, dy):
        pltpu.make_async_remote_copy(
            src_ref=arx.at[dy - 1, e], dst_ref=arx.at[dy - 1, e],
            send_sem=as_sem.at[dy - 1, e], recv_sem=ar_sem.at[dy - 1, e],
            device_id={"dp": dp_of(0, dy)}, device_id_type=MESH,
        ).wait_recv()

    acc[...] = jnp.zeros_like(acc)

    def logits_of(dx, dy):
        cols = a_cols(dx, dy)
        for h in range(2):
            d_wait(dx, dy, h)

        def step(n, carry):
            lanes = pl.ds(pl.multiple_of(n * 256, 256), 256)
            acc[:, lanes] += jnp.dot(
                a_v[:, pl.ds(cols, chip)], wbuf[pl.ds(cols, chip), lanes],
                preferred_element_type=F32,
            )
            return carry

        lax.fori_loop(0, width // 256, step, 0)

    w_send(0, 0, 0, 1, 0)
    w_send(0, 0, 0, 0, 1)
    w_send(0, 0, 1, 0, 3)
    w_send(0, 0, 1, 1, 0)
    w_send(0, 0, 1, 0, 1)
    w_send(0, 0, 0, 0, 3)
    w_pass(0, 0, 0)
    w_pass(0, 0, 1)
    load_a.wait()

    w_wait(0, 3, 0)
    w_send(0, 3, 0, 0, 1)
    w_send(0, 3, 0, 1, 0)
    w_pass(0, 3, 0)
    w_wait(0, 1, 1)
    w_send(0, 1, 1, 0, 3)
    w_send(0, 1, 1, 1, 0)
    w_pass(0, 1, 1)
    w_wait(1, 0, 0)
    w_send(1, 0, 0, 0, 3)
    w_pass(1, 0, 0)
    w_wait(1, 0, 1)
    w_send(1, 0, 1, 0, 1)
    w_pass(1, 0, 1)
    for dy in (2, 1, 3):
        a_send(0, 1, dy)
    logits_of(0, 0)
    w_wait(0, 3, 1)
    w_pass(0, 3, 1)
    w_wait(0, 1, 0)
    w_pass(0, 1, 0)
    logits_of(1, 0)
    w_wait(0, 2, 0)
    w_send(0, 2, 0, 1, 0)
    w_pass(0, 2, 0)
    w_wait(0, 2, 1)
    w_send(0, 2, 1, 1, 0)
    w_pass(0, 2, 1)
    logits_of(0, 3)
    logits_of(0, 1)
    logits_of(0, 2)
    w_wait(1, 3, 1)
    w_pass(1, 3, 1)
    w_wait(1, 1, 0)
    w_pass(1, 1, 0)
    w_wait(1, 3, 0)
    w_pass(1, 3, 0)
    w_wait(1, 1, 1)
    w_pass(1, 1, 1)
    logits_of(1, 3)
    logits_of(1, 1)
    w_wait(1, 2, 0)
    w_pass(1, 2, 0)
    w_wait(1, 2, 1)
    w_pass(1, 2, 1)
    logits_of(1, 2)

    classes = lax.broadcasted_iota(jnp.int32, (128, width), 1)
    loss_lanes = jnp.zeros((1, 128), F32)
    for t in range(tok // 128):
        lab = jnp.broadcast_to(labels_ref[t : t + 1, :], (128, 128)).T
        lab = jnp.concatenate([lab] * (width // 128), axis=1)
        logits = acc[t * 128 : (t + 1) * 128, :]
        top = jnp.max(logits, axis=1, keepdims=True)
        exps = jnp.exp(logits - top)
        denom = jnp.sum(exps, axis=1, keepdims=True)
        onehot = (lab == classes).astype(F32)
        picked = jnp.sum(logits * onehot, axis=1, keepdims=True)
        probs = exps / denom
        slopes[0, t * 128 : (t + 1) * 128, :] = ((probs - onehot) / tokens).astype(BF16)
        term = top + jnp.log(denom) - picked
        loss_lanes += jnp.sum(jnp.broadcast_to(term, (128, 128)), axis=0, keepdims=True)

    for dy in (2, 1, 3):
        send(slopes.at[0], slopes.at[dy], ss_sem.at[dy - 1], sr_sem.at[dy - 1], dp_of(0, dy))
    for dy in (2, 1, 3):
        a_send(1, 0, dy)

    def s_wait(dy):
        pltpu.make_async_remote_copy(
            src_ref=slopes.at[dy], dst_ref=slopes.at[dy],
            send_sem=ss_sem.at[dy - 1], recv_sem=sr_sem.at[dy - 1],
            device_id={"dp": dp_of(0, dy)}, device_id_type=MESH,
        ).wait_recv()

    def outer(left, right):
        return lax.dot_general(
            left, right, (((0,), (0,)), ((), ())), preferred_element_type=F32
        )

    def accumulate(e, dx, dy, first, start, count):
        at = pl.multiple_of(start, 128)
        if dy == 0:
            left = a_v[:, pl.ds(pl.multiple_of(a_cols(dx, 0) + at, 128), count)]
        else:
            left = arx[dy - 1, e, :, pl.ds(at, count)]
        here = outer(left, slopes[dy])
        if first:
            part[e, pl.ds(at, count), :] = here
        else:
            part[e, pl.ds(at, count), :] += here

    mine = pl.multiple_of(c * rows, 64)
    other = pl.multiple_of((1 - c) * rows, 64)
    big = (1 - c) * 384
    small = c * 512

    def exchange(e, h):
        return send(
            part.at[e, pl.ds(pl.multiple_of(other + h * half, 32), half), :],
            dbuf.at[e, pl.ds(h * half, half), :],
            es_sem.at[e, h], er_sem.at[e, h], dp_of(0, 0, 1),
        )

    accumulate(0, 1, 0, True, big, 512)
    for dy in (1, 3, 2):
        s_wait(dy)
        a_wait(0, dy)
        accumulate(0, 1, dy, False, big, 512)
    swaps = [exchange(0, h) for h in range(2)]
    for dy in (0, 1, 3, 2):
        accumulate(0, 1, dy, dy == 0, small, 384)
    xs = []
    for h in range(2):
        swaps[h].wait_recv()
        piece = pl.ds(h * half, half)
        xsend[piece, :] = part[0, pl.ds(pl.multiple_of(mine + h * half, 32), half), :] + dbuf[0, piece, :]
        xs.append(send(xsend.at[piece, :], xrecv.at[piece, :], xs_sem.at[h], xr_sem.at[h], dp_of(1, 0)))

    for dy in (0, 2, 1, 3):
        if dy:
            a_wait(1, dy)
        accumulate(1, 0, dy, dy == 0, big, 512)
        if dy != 3:
            accumulate(1, 0, dy, dy == 0, small, 384)
    swaps = [exchange(1, h) for h in range(2)]
    accumulate(1, 0, 3, False, small, 384)
    for h in range(2):
        swaps[h].wait_recv()
    for h in range(2):
        xs[h].wait_recv()

    def finish(g, carry):
        r = pl.multiple_of(g * 8, 8)
        m = pl.multiple_of(mine + g * 8, 8)
        for j in range(4):
            lanes = slice(j * 128, (j + 1) * 128)
            v = part[1, pl.ds(m, 8), lanes] + dbuf[1, pl.ds(r, 8), lanes] + xrecv[pl.ds(r, 8), lanes]
            grad_ref[pl.ds(g * 32 + j, 8, stride=4), :] = v
            carry = carry + v * v
        return carry

    square = lax.fori_loop(0, rows // 8, finish, jnp.zeros((8, 128), F32))
    tile = jnp.concatenate(
        [jnp.sum(square, axis=0, keepdims=True), loss_lanes, jnp.zeros((6, 128), F32)], axis=0
    )
    slots1[d] = tile
    first = []
    for k in range(1, 16):
        cp = pltpu.make_async_remote_copy(
            src_ref=slots1.at[d], dst_ref=slots1.at[d], send_sem=p1s.at[k - 1],
            recv_sem=p1r.at[k - 1], device_id={"dp": (d + k) % 16}, device_id_type=MESH,
        )
        cp.start()
        first.append(cp)
    for cp in first:
        cp.wait()
    slots2[lay] = jnp.sum(slots1[...], axis=0)
    second = []
    for k in range(1, 8):
        cp = pltpu.make_async_remote_copy(
            src_ref=slots2.at[lay], dst_ref=slots2.at[lay], send_sem=p2s.at[k - 1],
            recv_sem=p2r.at[k - 1], device_id={"layer": (lay + k) % 8}, device_id_type=MESH,
        )
        cp.start()
        second.append(cp)
    for cp in second:
        cp.wait()
    sums_ref[...] = jnp.sum(slots2[...], axis=0)
    for cp in sent:
        cp.wait_send()


def shards(activations, labels, weights, first_moment, second_moment):
    tok = activations.shape[0]
    depth = activations.shape[2]
    rows, _, width = weights.shape
    tokens = tok * lax.axis_size("dp")
    layers = lax.axis_size("layer")
    dma = pltpu.SemaphoreType.DMA
    vmem = pltpu.VMEM
    lines = rows * width // 128
    anywhere = pl.BlockSpec(memory_space=pl.ANY)
    inside = pl.BlockSpec(memory_space=pltpu.VMEM)

    def body(*refs):
        kernel(tokens, *refs)

    grad, sums = pl.pallas_call(
        body,
        out_shape=(
            jax.ShapeDtypeStruct((lines, 128), F32),
            jax.ShapeDtypeStruct((8, 128), F32),
        ),
        in_specs=[anywhere, inside, anywhere],
        out_specs=(inside, inside),
        scratch_shapes=[
            vmem((tok, depth), BF16),
            vmem((lines, 128), F32),
            vmem((depth, width), BF16),
            vmem((3, 2, tok, 2 * rows), BF16),
            vmem((4, tok, width), BF16),
            vmem((tok, width), F32),
            vmem((2, 2 * rows, width), F32),
            vmem((2, rows, width), F32),
            vmem((rows, width), F32),
            vmem((rows, width), F32),
            vmem((16, 8, 128), F32),
            vmem((8, 8, 128), F32),
            dma((2,)),
            dma((14,)),
            dma((8, 2)),
            dma((8, 2)),
            dma((8, 2)),
            dma((3, 2)),
            dma((3, 2)),
            dma((3,)),
            dma((3,)),
            dma((2, 2)),
            dma((2, 2)),
            dma((2,)),
            dma((2,)),
            dma((15,)),
            dma((15,)),
            dma((7,)),
            dma((7,)),
        ],
        compiler_params=pltpu.CompilerParams(
            collective_id=0, has_side_effects=True, vmem_limit_bytes=48 << 20
        ),
        name="probe_step",
    )(
        activations.reshape(tok, depth),
        labels.reshape(tok // 128, 128),
        weights.reshape(lines, 128),
    )
    square = jnp.sum(sums[0])
    loss = sums[1, 0] / (tokens * layers)
    grad = grad.reshape(rows, 1, width)
    factor = jnp.minimum(1.0, 0.25 / jnp.sqrt(square + 1e-12))
    clipped = factor * grad
    new_first = 0.9 * first_moment + 0.1 * clipped
    new_second = 0.999 * second_moment + 0.001 * clipped * clipped
    new_weights = weights - 0.001 * (new_first / (1.0 - 0.9**STEP)) / (
        jnp.sqrt(new_second / (1.0 - 0.999**STEP)) + 1e-08
    )
    return (new_weights, new_first, new_second, loss)


def solution(mesh):
    rows = P("dp", "layer", None)
    return jax.shard_map(
        shards,
        mesh=mesh,
        in_specs=(rows, P("dp"), rows, rows, rows),
        out_specs=(rows, rows, rows, P()),
        check_vma=False,
    )
```

```python
import jax
import jax.numpy as jnp
from jax import lax
from jax.experimental import pallas as pl
from jax.experimental.pallas import tpu as pltpu
from jax.sharding import PartitionSpec as P

STEP = 10
BF16 = jnp.bfloat16
F32 = jnp.float32
MESH = pl.DeviceIdType.MESH


def kernel(
    tokens,
    a_hbm,
    labels_hbm,
    w_hbm,
    grad_ref,
    factor_ref,
    loss_ref,
    a_v,
    labels_ref,
    w32,
    wbuf,
    arx,
    slopes,
    acc,
    part,
    dbuf,
    xsend,
    xrecv,
    slots1,
    slots2,
    ld_sem,
    ws_sem,
    wr_sem,
    ds_sem,
    dr_sem,
    as_sem,
    ar_sem,
    ss_sem,
    sr_sem,
    es_sem,
    er_sem,
    xs_sem,
    xr_sem,
    p1s,
    p1r,
    p2s,
    p2r,
    mid1,
    mid2,
):
    tok = a_v.shape[0]
    width = wbuf.shape[1]
    rows = wbuf.shape[0] // 16
    half = rows // 2
    chip = 2 * rows
    d = lax.axis_index("dp")
    lay = lax.axis_index("layer")
    x = d // 8
    y = (d // 2) % 4
    c = d % 2

    def dp_of(dx, dy, dc=0):
        return ((x + dx) % 2) * 8 + ((y + dy) % 4) * 2 + (c + dc) % 2

    load_a = pltpu.make_async_copy(a_hbm, a_v, ld_sem.at[0])
    load_w = pltpu.make_async_copy(w_hbm, w32, ld_sem.at[1])
    load_labels = pltpu.make_async_copy(labels_hbm, labels_ref, ld_sem.at[2])
    load_w.start()
    load_a.start()
    load_labels.start()

    away = (lay + 4) % 8
    z_next, z_last = (lay // 4 * 4 + (lay + k) % 4 for k in (1, 3))
    near = [
        {"dp": dp_of(1, 0)},
        {"dp": dp_of(1, 0), "layer": away},
        {"dp": dp_of(0, 1)},
        {"dp": dp_of(0, 3)},
        {"dp": dp_of(0, 0, 1)},
        {"layer": z_next},
        {"layer": z_last},
    ]
    barrier = pltpu.get_barrier_semaphore()
    for who in near:
        pl.semaphore_signal(barrier, inc=1, device_id=who, device_id_type=MESH)

    with jax.named_scope("start"):
        load_w.wait()
        own = pl.multiple_of(d * rows, 64)

        def convert(g, carry):
            for j in range(4):
                v = w32[pl.ds(g * 64 + j, 16, stride=4), :]
                wbuf[pl.ds(pl.multiple_of(own + g * 16, 16), 16), j * 128 : (j + 1) * 128] = v.astype(BF16)
            return carry

        lax.fori_loop(0, rows // 16, convert, 0)
        with jax.named_scope("barrier"):
            pl.semaphore_wait(barrier, len(near))

    sent = []

    def send(src, dst, ssem, rsem, dp):
        cp = pltpu.make_async_remote_copy(
            src_ref=src, dst_ref=dst, send_sem=ssem, recv_sem=rsem,
            device_id={"dp": dp}, device_id_type=MESH,
        )
        cp.start()
        sent.append(cp)
        return cp

    def w_rows(dx, dy, dc, h):
        start = pl.multiple_of(dp_of(dx, dy, dc) * rows + h * half, 32)
        return wbuf.at[pl.ds(start, half), :]

    wcount = [0]

    def w_send(dx, dy, h, tx, ty):
        ref = w_rows(dx, dy, 0, h)
        k = ((dx - tx) % 2) * 4 + (dy - ty) % 4
        i = wcount[0]
        wcount[0] += 1
        send(ref, ref, ws_sem.at[i], wr_sem.at[k, h], dp_of(tx, ty))

    def w_pass(dx, dy, h):
        ref = w_rows(dx, dy, 0, h)
        k = dx * 4 + dy
        send(ref, ref, ds_sem.at[k, h], dr_sem.at[k, h], dp_of(0, 0, 1))

    def w_wait(dx, dy, h):
        ref = w_rows(dx, dy, 0, h)
        pltpu.make_async_remote_copy(
            src_ref=ref, dst_ref=ref, send_sem=ws_sem.at[0], recv_sem=wr_sem.at[dx * 4 + dy, h],
            device_id={"dp": dp_of(0, 0, 1)}, device_id_type=MESH,
        ).wait_recv()

    def d_wait(dx, dy, h):
        ref = w_rows(dx, dy, 1, h)
        pltpu.make_async_remote_copy(
            src_ref=ref, dst_ref=ref, send_sem=ws_sem.at[0], recv_sem=dr_sem.at[dx * 4 + dy, h],
            device_id={"dp": dp_of(0, 0, 1)}, device_id_type=MESH,
        ).wait_recv()

    def a_cols(dx, dy):
        return pl.multiple_of((((x + dx) % 2) * 4 + (y + dy) % 4) * chip, 128)

    cuts = (pl.ds(0, 256), pl.ds(256, chip - 256))

    def a_send(e, dx, dy, part):
        cut = cuts[part]
        send(
            a_hbm.at[:, pl.ds(pl.multiple_of(a_cols(dx, dy) + cut.start, 128), cut.size)],
            arx.at[dy - 1, e, :, cut],
            as_sem.at[dy - 1, e, part], ar_sem.at[dy - 1, e, part], dp_of(0, dy),
        )

    def a_wait(e, dy):
        for part, cut in enumerate(cuts):
            ref = arx.at[dy - 1, e, :, cut]
            pltpu.make_async_remote_copy(
                src_ref=ref, dst_ref=ref,
                send_sem=as_sem.at[dy - 1, e, part], recv_sem=ar_sem.at[dy - 1, e, part],
                device_id={"dp": dp_of(0, dy)}, device_id_type=MESH,
            ).wait_recv()

    acc[...] = jnp.zeros_like(acc)

    def logits_of(dx, dy):
        cols = a_cols(dx, dy)
        for h in range(2):
            d_wait(dx, dy, h)

        def step(n, carry):
            lanes = pl.ds(pl.multiple_of(n * 256, 256), 256)
            acc[:, lanes] += jnp.dot(
                a_v[:, pl.ds(cols, chip)], wbuf[pl.ds(cols, chip), lanes],
                preferred_element_type=F32,
            )
            return carry

        lax.fori_loop(0, width // 256, step, 0)

    for who in near[-2:]:
        pl.semaphore_signal(mid1, inc=1, device_id=who, device_id_type=MESH)
    with jax.named_scope("own"):
        w_send(0, 0, 0, 1, 0)
        w_send(0, 0, 0, 0, 1)
        w_send(0, 0, 1, 0, 3)
        w_send(0, 0, 1, 1, 0)
        w_send(0, 0, 1, 0, 1)
        w_send(0, 0, 0, 0, 3)
        w_pass(0, 0, 0)
        w_pass(0, 0, 1)
        load_a.wait()
        load_labels.wait()

    with jax.named_scope("relay1"):
        w_wait(0, 3, 0)
        w_send(0, 3, 0, 0, 1)
        w_send(0, 3, 0, 1, 0)
        w_pass(0, 3, 0)
        w_wait(0, 1, 1)
        w_send(0, 1, 1, 0, 3)
        w_send(0, 1, 1, 1, 0)
        w_pass(0, 1, 1)
        w_wait(1, 0, 0)
        w_send(1, 0, 0, 0, 3)
        w_pass(1, 0, 0)
        w_wait(1, 0, 1)
        w_send(1, 0, 1, 0, 1)
        w_pass(1, 0, 1)

    for dy in (2, 1, 3):
        for cut in range(2):
            a_send(0, 1, dy, cut)
    with jax.named_scope("log1"):
        logits_of(0, 0)
        w_wait(0, 3, 1)
        w_pass(0, 3, 1)
        w_wait(0, 1, 0)
        w_pass(0, 1, 0)
        logits_of(1, 0)

    with jax.named_scope("log2"):
        w_wait(0, 2, 0)
        w_send(0, 2, 0, 1, 0)
        w_pass(0, 2, 0)
        w_wait(0, 2, 1)
        w_send(0, 2, 1, 1, 0)
        w_pass(0, 2, 1)
        logits_of(0, 3)
        logits_of(0, 1)
        logits_of(0, 2)

    with jax.named_scope("log3"):
        w_wait(1, 3, 1)
        w_pass(1, 3, 1)
        w_wait(1, 1, 0)
        w_pass(1, 1, 0)
        w_wait(1, 3, 0)
        w_pass(1, 3, 0)
        w_wait(1, 1, 1)
        w_pass(1, 1, 1)
        logits_of(1, 3)
        logits_of(1, 1)

    with jax.named_scope("log4"):
        w_wait(1, 2, 0)
        w_pass(1, 2, 0)
        w_wait(1, 2, 1)
        w_pass(1, 2, 1)
        logits_of(1, 2)

    with jax.named_scope("softmax"):
        classes = lax.broadcasted_iota(jnp.int32, (128, width), 1)
        loss_lanes = jnp.zeros((1, 128), F32)
        for t in range(tok // 128):
            lab = jnp.broadcast_to(labels_ref[t : t + 1, :], (128, 128)).T
            lab = jnp.concatenate([lab] * (width // 128), axis=1)
            logits = acc[t * 128 : (t + 1) * 128, :]
            top = jnp.max(logits, axis=1, keepdims=True)
            exps = jnp.exp(logits - top)
            denom = jnp.sum(exps, axis=1, keepdims=True)
            onehot = (lab == classes).astype(F32)
            picked = jnp.sum(logits * onehot, axis=1, keepdims=True)
            probs = exps / denom
            slopes[0, t * 128 : (t + 1) * 128, :] = ((probs - onehot) / tokens).astype(BF16)
            term = top + jnp.log(denom) - picked
            loss_lanes += jnp.sum(jnp.broadcast_to(term, (128, 128)), axis=0, keepdims=True)

    def slope_send(src, dy, rows, i, k):
        send(
            slopes.at[src, rows, :], slopes.at[(src + dy) % 4, rows, :],
            ss_sem.at[i], sr_sem.at[k], dp_of(0, dy),
        )

    def slope_wait(slot, rows, k):
        pltpu.make_async_remote_copy(
            src_ref=slopes.at[slot, rows, :], dst_ref=slopes.at[slot, rows, :],
            send_sem=ss_sem.at[0], recv_sem=sr_sem.at[k],
            device_id={"dp": dp_of(0, 1)}, device_id_type=MESH,
        ).wait_recv()

    every, upper, lower = pl.ds(0, tok), pl.ds(0, tok // 2), pl.ds(tok // 2, tok // 2)
    slope_send(0, 1, every, 0, 0)
    slope_send(0, 3, every, 1, 1)
    for dy in (1, 3):
        a_send(1, 0, dy, 0)
    pl.semaphore_wait(mid1, 2)
    pl.semaphore_signal(mid2, inc=1, device_id={"layer": away}, device_id_type=MESH)

    def outer(left, right):
        return lax.dot_general(
            left, right, (((0,), (0,)), ((), ())), preferred_element_type=F32
        )

    def accumulate(e, dx, dy, first, start, count):
        at = pl.multiple_of(start, 128)
        if dy == 0:
            left = a_v[:, pl.ds(pl.multiple_of(a_cols(dx, 0) + at, 128), count)]
        else:
            left = arx[dy - 1, e, :, pl.ds(at, count)]
        here = outer(left, slopes[dy])
        if first:
            part[e, pl.ds(at, count), :] = here
        else:
            part[e, pl.ds(at, count), :] += here

    mine = pl.multiple_of(c * rows, 64)
    other = pl.multiple_of((1 - c) * rows, 64)
    big = (1 - c) * 384
    small = c * 512

    def exchange(e, h):
        return send(
            part.at[e, pl.ds(pl.multiple_of(other + h * half, 32), half), :],
            dbuf.at[e, pl.ds(h * half, half), :],
            es_sem.at[e, h], er_sem.at[e, h], dp_of(0, 0, 1),
        )

    accumulate(0, 1, 0, True, big, 512)
    with jax.named_scope("slope1"):
        slope_wait(1, every, 0)
        slope_send(1, 1, upper, 2, 2)
        slope_wait(3, every, 1)
        slope_send(3, 3, lower, 3, 3)
        a_send(1, 0, 2, 0)
        for dy in (1, 3, 2):
            a_send(1, 0, dy, 1)
    with jax.named_scope("gradx1"):
        for dy in (1, 3):
            a_wait(0, dy)
            accumulate(0, 1, dy, False, big, 512)
    with jax.named_scope("slope2"):
        slope_wait(2, upper, 2)
        slope_wait(2, lower, 3)
    with jax.named_scope("gradx1b"):
        a_wait(0, 2)
        accumulate(0, 1, 2, False, big, 512)

    with jax.named_scope("gradx2"):
        swaps = [exchange(0, h) for h in range(2)]
        for dy in (0, 1, 3, 2):
            accumulate(0, 1, dy, dy == 0, small, 384)
        xs = []
        for h in range(2):
            swaps[h].wait_recv()
            piece = pl.ds(h * half, half)
            xsend[piece, :] = part[0, pl.ds(pl.multiple_of(mine + h * half, 32), half), :] + dbuf[0, piece, :]
            xs.append(send(xsend.at[piece, :], xrecv.at[piece, :], xs_sem.at[h], xr_sem.at[h], dp_of(1, 0)))

    with jax.named_scope("grado1"):
        for dy in (0, 2, 1, 3):
            if dy:
                a_wait(1, dy)
            accumulate(1, 0, dy, dy == 0, big, 512)
            if dy != 3:
                accumulate(1, 0, dy, dy == 0, small, 384)

    with jax.named_scope("grado2"):
        swaps = [exchange(1, h) for h in range(2)]
        accumulate(1, 0, 3, False, small, 384)
        for h in range(2):
            swaps[h].wait_recv()

    with jax.named_scope("xwait"):
        for h in range(2):
            xs[h].wait_recv()

    def finish(g, carry):
        r = pl.multiple_of(g * 8, 8)
        m = pl.multiple_of(mine + g * 8, 8)
        for j in range(4):
            lanes = slice(j * 128, (j + 1) * 128)
            v = part[1, pl.ds(m, 8), lanes] + dbuf[1, pl.ds(r, 8), lanes] + xrecv[pl.ds(r, 8), lanes]
            grad_ref[pl.ds(g * 32 + j, 8, stride=4), :] = v
            carry = carry + v * v
        return carry

    with jax.named_scope("fin"):
        square = lax.fori_loop(0, rows // 8, finish, jnp.zeros((8, 128), F32))
        tile = jnp.concatenate(
            [jnp.sum(square, axis=0, keepdims=True), loss_lanes, jnp.zeros((6, 128), F32)], axis=0
        )

    with jax.named_scope("red1"):
        slots1[d] = tile
        first = []
        for k in range(1, 16):
            cp = pltpu.make_async_remote_copy(
                src_ref=slots1.at[d], dst_ref=slots1.at[d], send_sem=p1s.at[k - 1],
                recv_sem=p1r.at[k - 1], device_id={"dp": (d + k) % 16}, device_id_type=MESH,
            )
            cp.start()
            first.append(cp)
        for cp in first:
            cp.wait()

    with jax.named_scope("red2"):
        pl.semaphore_wait(mid2, 1)
        slots2[lay] = jnp.sum(slots1[...], axis=0)
        second = []
        for k in range(1, 8):
            cp = pltpu.make_async_remote_copy(
                src_ref=slots2.at[lay], dst_ref=slots2.at[lay], send_sem=p2s.at[k - 1],
                recv_sem=p2r.at[k - 1], device_id={"layer": (lay + k) % 8}, device_id_type=MESH,
            )
            cp.start()
            second.append(cp)
        for cp in second:
            cp.wait()

    sums = jnp.sum(slots2[...], axis=0)
    square = jnp.broadcast_to(jnp.sum(sums[0:1, :], axis=1, keepdims=True), (1, 128))
    factor_ref[...] = jnp.minimum(1.0, 0.25 / jnp.sqrt(square + 1e-12))
    loss_ref[...] = sums[1:2, :] / (tokens * 8)
    for cp in sent:
        cp.wait_send()


def shards(activations, labels, weights, first_moment, second_moment):
    tok = activations.shape[0]
    depth = activations.shape[2]
    rows, _, width = weights.shape
    tokens = tok * lax.axis_size("dp")
    dma = pltpu.SemaphoreType.DMA
    vmem = pltpu.VMEM
    lines = rows * width // 128
    anywhere = pl.BlockSpec(memory_space=pltpu.MemorySpace.HBM)
    inside = pl.BlockSpec(memory_space=pltpu.VMEM)

    def body(*refs):
        kernel(tokens, *refs)

    grad, factor, loss = pl.pallas_call(
        body,
        out_shape=(
            jax.ShapeDtypeStruct((lines, 128), F32),
            jax.ShapeDtypeStruct((1, 128), F32),
            jax.ShapeDtypeStruct((1, 128), F32),
        ),
        in_specs=[anywhere, anywhere, anywhere],
        out_specs=(inside, inside, inside),
        scratch_shapes=[
            vmem((tok, depth), BF16),
            vmem((tok // 128, 128), jnp.int32),
            vmem((lines, 128), F32),
            vmem((depth, width), BF16),
            vmem((3, 2, tok, 2 * rows), BF16),
            vmem((4, tok, width), BF16),
            vmem((tok, width), F32),
            vmem((2, 2 * rows, width), F32),
            vmem((2, rows, width), F32),
            vmem((rows, width), F32),
            vmem((rows, width), F32),
            vmem((16, 8, 128), F32),
            vmem((8, 8, 128), F32),
            dma((3,)),
            dma((14,)),
            dma((8, 2)),
            dma((8, 2)),
            dma((8, 2)),
            dma((3, 2, 2)),
            dma((3, 2, 2)),
            dma((4,)),
            dma((4,)),
            dma((2, 2)),
            dma((2, 2)),
            dma((2,)),
            dma((2,)),
            dma((15,)),
            dma((15,)),
            dma((7,)),
            dma((7,)),
            pltpu.SemaphoreType.REGULAR,
            pltpu.SemaphoreType.REGULAR,
        ],
        compiler_params=pltpu.CompilerParams(
            collective_id=0, has_side_effects=True, vmem_limit_bytes=48 << 20
        ),
        name="probe_step",
    )(
        *(
            pltpu.with_memory_space_constraint(v, pltpu.MemorySpace.HBM)
            for v in (
                activations.reshape(tok, depth),
                labels.reshape(tok // 128, 128),
                weights.reshape(lines, 128),
            )
        )
    )
    held = [v.reshape(lines, 128) for v in (weights, first_moment, second_moment)]
    grad, weights, first_moment, second_moment = lax.optimization_barrier((grad, *held))
    clipped = factor * grad
    new_first = 0.9 * first_moment + 0.1 * clipped
    new_second = 0.999 * second_moment + 0.001 * clipped * clipped
    new_weights = weights - 0.001 * (new_first / (1.0 - 0.9**STEP)) / (
        jnp.sqrt(new_second / (1.0 - 0.999**STEP)) + 1e-08
    )
    outs = (v.reshape(rows, 1, width) for v in (new_weights, new_first, new_second))
    return (*outs, loss[0, 0])


def solution(mesh):
    rows = P("dp", "layer", None)
    return jax.shard_map(
        shards,
        mesh=mesh,
        in_specs=(rows, P("dp"), rows, rows, rows),
        out_specs=(rows, rows, rows, P()),
        check_vma=False,
    )
```

```python
import jax
import jax.numpy as jnp
from jax import lax
from jax.experimental import pallas as pl
from jax.experimental.pallas import tpu as pltpu
from jax.sharding import PartitionSpec as P

STEP = 10
BF16 = jnp.bfloat16
F32 = jnp.float32
MESH = pl.DeviceIdType.MESH


def kernel(
    tokens,
    a_hbm,
    labels_hbm,
    w_hbm,
    grad_ref,
    factor_ref,
    loss_ref,
    a_v,
    labels_ref,
    w32,
    wbuf,
    arx,
    slopes,
    acc,
    part,
    dbuf,
    xsend,
    xrecv,
    slots1,
    slots2,
    ld_sem,
    ws_sem,
    wr_sem,
    ds_sem,
    dr_sem,
    as_sem,
    ar_sem,
    ss_sem,
    sr_sem,
    es_sem,
    er_sem,
    xs_sem,
    xr_sem,
    p1s,
    p1r,
    p2s,
    p2r,
    mid1,
    mid2,
):
    tok = a_v.shape[0]
    width = wbuf.shape[1]
    rows = wbuf.shape[0] // 16
    half = rows // 2
    chip = 2 * rows
    d = lax.axis_index("dp")
    lay = lax.axis_index("layer")
    x = d // 8
    y = (d // 2) % 4
    c = d % 2

    def dp_of(dx, dy, dc=0):
        return ((x + dx) % 2) * 8 + ((y + dy) % 4) * 2 + (c + dc) % 2

    load_a = pltpu.make_async_copy(a_hbm, a_v, ld_sem.at[0])
    load_w = pltpu.make_async_copy(w_hbm, w32, ld_sem.at[1])
    load_labels = pltpu.make_async_copy(labels_hbm, labels_ref, ld_sem.at[2])
    load_w.start()
    load_a.start()
    load_labels.start()

    away = (lay + 4) % 8
    z_next, z_last = (lay // 4 * 4 + (lay + k) % 4 for k in (1, 3))
    near = [
        {"dp": dp_of(1, 0)},
        {"dp": dp_of(1, 0), "layer": away},
        {"dp": dp_of(0, 1)},
        {"dp": dp_of(0, 3)},
        {"dp": dp_of(0, 0, 1)},
        {"layer": z_next},
        {"layer": z_last},
    ]
    barrier = pltpu.get_barrier_semaphore()
    for who in near:
        pl.semaphore_signal(barrier, inc=1, device_id=who, device_id_type=MESH)

    with jax.named_scope("start"):
        load_w.wait()
        own = pl.multiple_of(d * rows, 64)

        def convert(g, carry):
            for j in range(4):
                v = w32[pl.ds(g * 64 + j, 16, stride=4), :]
                wbuf[pl.ds(pl.multiple_of(own + g * 16, 16), 16), j * 128 : (j + 1) * 128] = v.astype(BF16)
            return carry

        lax.fori_loop(0, rows // 16, convert, 0)
        with jax.named_scope("barrier"):
            pl.semaphore_wait(barrier, len(near))

    sent = []

    def send(src, dst, ssem, rsem, dp):
        cp = pltpu.make_async_remote_copy(
            src_ref=src, dst_ref=dst, send_sem=ssem, recv_sem=rsem,
            device_id={"dp": dp}, device_id_type=MESH,
        )
        cp.start()
        sent.append(cp)
        return cp

    def w_rows(dx, dy, dc, h):
        start = pl.multiple_of(dp_of(dx, dy, dc) * rows + h * half, 32)
        return wbuf.at[pl.ds(start, half), :]

    wcount = [0]

    def w_send(dx, dy, h, tx, ty):
        ref = w_rows(dx, dy, 0, h)
        k = ((dx - tx) % 2) * 4 + (dy - ty) % 4
        i = wcount[0]
        wcount[0] += 1
        send(ref, ref, ws_sem.at[i], wr_sem.at[k, h], dp_of(tx, ty))

    def w_pass(dx, dy, h):
        ref = w_rows(dx, dy, 0, h)
        k = dx * 4 + dy
        send(ref, ref, ds_sem.at[k, h], dr_sem.at[k, h], dp_of(0, 0, 1))

    def w_wait(dx, dy, h):
        ref = w_rows(dx, dy, 0, h)
        pltpu.make_async_remote_copy(
            src_ref=ref, dst_ref=ref, send_sem=ws_sem.at[0], recv_sem=wr_sem.at[dx * 4 + dy, h],
            device_id={"dp": dp_of(0, 0, 1)}, device_id_type=MESH,
        ).wait_recv()

    def d_wait(dx, dy, h):
        ref = w_rows(dx, dy, 1, h)
        pltpu.make_async_remote_copy(
            src_ref=ref, dst_ref=ref, send_sem=ws_sem.at[0], recv_sem=dr_sem.at[dx * 4 + dy, h],
            device_id={"dp": dp_of(0, 0, 1)}, device_id_type=MESH,
        ).wait_recv()

    def a_cols(dx, dy):
        return pl.multiple_of((((x + dx) % 2) * 4 + (y + dy) % 4) * chip, 128)

    cuts = ((0, 256), (640, 256), (256, 128), (384, 128), (512, 128))

    def a_send(e, dx, dy, k):
        start, size = cuts[k]
        send(
            a_hbm.at[:, pl.ds(pl.multiple_of(a_cols(dx, dy) + start, 128), size)],
            arx.at[dy - 1, e, :, pl.ds(start, size)],
            as_sem.at[dy - 1, e, k], ar_sem.at[dy - 1, e, k], dp_of(0, dy),
        )

    def a_wait(e, dy, which):
        for k in which:
            ref = arx.at[dy - 1, e, :, pl.ds(*cuts[k])]
            pltpu.make_async_remote_copy(
                src_ref=ref, dst_ref=ref,
                send_sem=as_sem.at[dy - 1, e, k], recv_sem=ar_sem.at[dy - 1, e, k],
                device_id={"dp": dp_of(0, dy)}, device_id_type=MESH,
            ).wait_recv()

    ends, middle = (0, 1), (2, 3, 4)

    acc[...] = jnp.zeros_like(acc)

    def logits_of(dx, dy):
        cols = a_cols(dx, dy)
        for h in range(2):
            d_wait(dx, dy, h)

        def step(n, carry):
            lanes = pl.ds(pl.multiple_of(n * 256, 256), 256)
            acc[:, lanes] += jnp.dot(
                a_v[:, pl.ds(cols, chip)], wbuf[pl.ds(cols, chip), lanes],
                preferred_element_type=F32,
            )
            return carry

        lax.fori_loop(0, width // 256, step, 0)

    for who in near[-2:]:
        pl.semaphore_signal(mid1, inc=1, device_id=who, device_id_type=MESH)
    with jax.named_scope("own"):
        w_send(0, 0, 0, 1, 0)
        w_send(0, 0, 0, 0, 1)
        w_send(0, 0, 1, 0, 3)
        w_send(0, 0, 1, 1, 0)
        w_send(0, 0, 1, 0, 1)
        w_send(0, 0, 0, 0, 3)
        w_pass(0, 0, 0)
        w_pass(0, 0, 1)
        load_a.wait()
        load_labels.wait()

    with jax.named_scope("relay1"):
        w_wait(0, 3, 0)
        w_send(0, 3, 0, 0, 1)
        w_send(0, 3, 0, 1, 0)
        w_pass(0, 3, 0)
        w_wait(0, 1, 1)
        w_send(0, 1, 1, 0, 3)
        w_send(0, 1, 1, 1, 0)
        w_pass(0, 1, 1)
        w_wait(1, 0, 0)
        w_send(1, 0, 0, 0, 3)
        w_pass(1, 0, 0)
        w_wait(1, 0, 1)
        w_send(1, 0, 1, 0, 1)
        w_pass(1, 0, 1)

    with jax.named_scope("log1"):
        logits_of(0, 0)
        w_wait(0, 3, 1)
        w_pass(0, 3, 1)
        w_wait(0, 1, 0)
        w_pass(0, 1, 0)
        logits_of(1, 0)

    with jax.named_scope("log2"):
        w_wait(0, 2, 0)
        w_send(0, 2, 0, 1, 0)
        w_pass(0, 2, 0)
        w_wait(0, 2, 1)
        w_send(0, 2, 1, 1, 0)
        w_pass(0, 2, 1)
        logits_of(0, 3)
        logits_of(0, 1)
        logits_of(0, 2)

    for k in (0, 1, 2):
        for dy in (2, 1, 3):
            a_send(0, 1, dy, k)
    with jax.named_scope("log3"):
        w_wait(1, 3, 1)
        w_pass(1, 3, 1)
        w_wait(1, 1, 0)
        w_pass(1, 1, 0)
        w_wait(1, 3, 0)
        w_pass(1, 3, 0)
        w_wait(1, 1, 1)
        w_pass(1, 1, 1)
        logits_of(1, 3)
        logits_of(1, 1)

    with jax.named_scope("log4"):
        w_wait(1, 2, 0)
        w_pass(1, 2, 0)
        w_wait(1, 2, 1)
        w_pass(1, 2, 1)
        logits_of(1, 2)

    with jax.named_scope("softmax"):
        classes = lax.broadcasted_iota(jnp.int32, (128, width), 1)
        loss_lanes = jnp.zeros((1, 128), F32)
        for t in range(tok // 128):
            lab = jnp.broadcast_to(labels_ref[t : t + 1, :], (128, 128)).T
            lab = jnp.concatenate([lab] * (width // 128), axis=1)
            logits = acc[t * 128 : (t + 1) * 128, :]
            top = jnp.max(logits, axis=1, keepdims=True)
            exps = jnp.exp(logits - top)
            denom = jnp.sum(exps, axis=1, keepdims=True)
            onehot = (lab == classes).astype(F32)
            picked = jnp.sum(logits * onehot, axis=1, keepdims=True)
            probs = exps / denom
            slopes[0, t * 128 : (t + 1) * 128, :] = ((probs - onehot) / tokens).astype(BF16)
            term = top + jnp.log(denom) - picked
            loss_lanes += jnp.sum(jnp.broadcast_to(term, (128, 128)), axis=0, keepdims=True)

    def slope_send(src, dy, rows, i, k):
        send(
            slopes.at[src, rows, :], slopes.at[(src + dy) % 4, rows, :],
            ss_sem.at[i], sr_sem.at[k], dp_of(0, dy),
        )

    def slope_wait(slot, rows, k):
        pltpu.make_async_remote_copy(
            src_ref=slopes.at[slot, rows, :], dst_ref=slopes.at[slot, rows, :],
            send_sem=ss_sem.at[0], recv_sem=sr_sem.at[k],
            device_id={"dp": dp_of(0, 1)}, device_id_type=MESH,
        ).wait_recv()

    every, upper, lower = pl.ds(0, tok), pl.ds(0, tok // 2), pl.ds(tok // 2, tok // 2)
    slope_send(0, 1, every, 0, 0)
    slope_send(0, 3, every, 1, 1)
    left_here = [sent.pop(), sent.pop()]
    pl.semaphore_wait(mid1, 2)
    pl.semaphore_signal(mid2, inc=1, device_id={"layer": away}, device_id_type=MESH)

    def outer(left, right):
        return lax.dot_general(
            left, right, (((0,), (0,)), ((), ())), preferred_element_type=F32
        )

    def accumulate(e, dy, start, count):
        at = start if isinstance(start, int) else pl.multiple_of(start, 128)
        if dy == 0:
            left = a_v[:, pl.ds(pl.multiple_of(a_cols(1 - e, 0) + at, 128), count)]
        else:
            left = arx[dy - 1, e, :, pl.ds(at, count)]
        here = outer(left, slopes[dy])
        if dy == 0:
            part[e, pl.ds(at, count), :] = here
        else:
            part[e, pl.ds(at, count), :] += here

    groups = (
        (lambda k: k * 640, lambda k: k * 192, 256),
        (lambda k: 256 + k * 192, lambda k: (1 - k) * 256, 192),
    )

    def in_part(g, k):
        return pl.ds(pl.multiple_of(groups[g][0](k), 64), groups[g][2])

    def in_block(g, k):
        return pl.ds(pl.multiple_of(groups[g][1](k), 64), groups[g][2])

    def exchange(e, g):
        return send(
            part.at[e, in_part(g, 1 - c), :], dbuf.at[e, in_block(g, 1 - c), :],
            es_sem.at[e, g], er_sem.at[e, g], dp_of(0, 0, 1),
        )

    def swap_wait(e, g):
        ref = dbuf.at[e, in_block(g, c), :]
        pltpu.make_async_remote_copy(
            src_ref=ref, dst_ref=ref, send_sem=es_sem.at[e, g], recv_sem=er_sem.at[e, g],
            device_id={"dp": dp_of(0, 0, 1)}, device_id_type=MESH,
        ).wait_recv()

    def x_send(g):
        swap_wait(0, g)
        block = in_block(g, c)
        xsend[block, :] = part[0, in_part(g, c), :] + dbuf[0, block, :]
        return send(
            xsend.at[block, :], xrecv.at[block, :], xs_sem.at[g], xr_sem.at[g], dp_of(1, 0)
        )

    def finish(group, carry):
        swap_wait(1, group)
        size = groups[group][2]
        theirs, block = groups[group][0](c), groups[group][1](c)

        def step(g, carry):
            r = pl.multiple_of(block + g * 8, 8)
            m = pl.multiple_of(theirs + g * 8, 8)
            for j in range(4):
                lanes = slice(j * 128, (j + 1) * 128)
                v = part[1, pl.ds(m, 8), lanes] + dbuf[1, pl.ds(r, 8), lanes] + xrecv[pl.ds(r, 8), lanes]
                grad_ref[pl.ds(r * 4 + j, 8, stride=4), :] = v
                carry = carry + v * v
            return carry

        return lax.fori_loop(0, size // 8, step, carry)

    with jax.named_scope("grad0"):
        for e in range(2):
            accumulate(e, 0, 0, 512)
            accumulate(e, 0, 512, 384)
    with jax.named_scope("slopesent"):
        for cp in left_here:
            cp.wait_send()
        for dy in (2, 1, 3):
            a_send(0, 1, dy, 3)
    with jax.named_scope("slope1"):
        slope_wait(1, every, 0)
        slope_send(1, 1, upper, 2, 2)
        slope_wait(3, every, 1)
        slope_send(3, 3, lower, 3, 3)
        for dy in (2, 1, 3):
            a_send(0, 1, dy, 4)
    yours, mine = (1 - c) * 640, c * 640
    with jax.named_scope("gradx1"):
        for dy in (1, 3):
            a_wait(0, dy, ends)
            accumulate(0, dy, yours, 256)
            accumulate(0, dy, mine, 256)
    with jax.named_scope("slope2"):
        slope_wait(2, upper, 2)
        slope_wait(2, lower, 3)
    for which in (ends, middle):
        for k in which:
            for dy in (2, 1, 3):
                a_send(1, 0, dy, k)
    with jax.named_scope("gradx2"):
        a_wait(0, 2, ends)
        accumulate(0, 2, yours, 256)
        exchange(0, 0)
        accumulate(0, 2, mine, 256)
        pl.semaphore_wait(mid2, 1)
        xs = [x_send(0)]
    with jax.named_scope("gradx3"):
        for dy in (1, 3, 2):
            a_wait(0, dy, middle)
            accumulate(0, dy, 256, 384)
        exchange(0, 1)
        xs.append(x_send(1))
    with jax.named_scope("grado1"):
        for dy in (1, 3, 2):
            a_wait(1, dy, ends)
            accumulate(1, dy, yours, 256)
            accumulate(1, dy, mine, 256)
        exchange(1, 0)
    with jax.named_scope("fin1"):
        xs[0].wait_recv()
        square = finish(0, jnp.zeros((8, 128), F32))
    with jax.named_scope("grado2"):
        for dy in (1, 3, 2):
            a_wait(1, dy, middle)
            accumulate(1, dy, 256, 384)
        exchange(1, 1)
    with jax.named_scope("xwait"):
        xs[1].wait_recv()
    with jax.named_scope("fin2"):
        square = finish(1, square)
        tile = jnp.concatenate(
            [jnp.sum(square, axis=0, keepdims=True), loss_lanes, jnp.zeros((6, 128), F32)], axis=0
        )

    def spread(slots, here, index, peers, ssem, rsem):
        slots[index] = here
        copies = []
        for k, who in enumerate(peers):
            cp = pltpu.make_async_remote_copy(
                src_ref=slots.at[index], dst_ref=slots.at[index], send_sem=ssem.at[k],
                recv_sem=rsem.at[k], device_id=who, device_id_type=MESH,
            )
            cp.start()
            copies.append(cp)
        for cp in copies:
            cp.wait()
        return jnp.sum(slots[...], axis=0)

    m = y * 2 + c
    n = x * 8 + lay
    with jax.named_scope("red1"):
        tile = spread(
            slots1, tile, m, [{"dp": x * 8 + (m + k) % 8} for k in range(1, 8)], p1s, p1r
        )
    with jax.named_scope("red2"):
        others = [(n + k) % 16 for k in range(1, 16)]
        sums = spread(
            slots2, tile, n, [{"dp": o // 8 * 8 + m, "layer": o % 8} for o in others], p2s, p2r
        )
    square = jnp.broadcast_to(jnp.sum(sums[0:1, :], axis=1, keepdims=True), (1, 128))
    factor_ref[...] = jnp.minimum(1.0, 0.25 / jnp.sqrt(square + 1e-12))
    loss_ref[...] = sums[1:2, :] / (tokens * 8)
    for cp in sent:
        cp.wait_send()


def shards(activations, labels, weights, first_moment, second_moment):
    tok = activations.shape[0]
    depth = activations.shape[2]
    rows, _, width = weights.shape
    tokens = tok * lax.axis_size("dp")
    dma = pltpu.SemaphoreType.DMA
    vmem = pltpu.VMEM
    lines = rows * width // 128
    anywhere = pl.BlockSpec(memory_space=pltpu.MemorySpace.HBM)
    inside = pl.BlockSpec(memory_space=pltpu.VMEM)

    def body(*refs):
        kernel(tokens, *refs)

    grad, factor, loss = pl.pallas_call(
        body,
        out_shape=(
            jax.ShapeDtypeStruct((lines, 128), F32),
            jax.ShapeDtypeStruct((1, 128), F32),
            jax.ShapeDtypeStruct((1, 128), F32),
        ),
        in_specs=[anywhere, anywhere, anywhere],
        out_specs=(inside, inside, inside),
        scratch_shapes=[
            vmem((tok, depth), BF16),
            vmem((tok // 128, 128), jnp.int32),
            vmem((lines, 128), F32),
            vmem((depth, width), BF16),
            vmem((3, 2, tok, 2 * rows), BF16),
            vmem((4, tok, width), BF16),
            vmem((tok, width), F32),
            vmem((2, 2 * rows, width), F32),
            vmem((2, rows, width), F32),
            vmem((rows, width), F32),
            vmem((rows, width), F32),
            vmem((8, 8, 128), F32),
            vmem((16, 8, 128), F32),
            dma((3,)),
            dma((14,)),
            dma((8, 2)),
            dma((8, 2)),
            dma((8, 2)),
            dma((3, 2, 5)),
            dma((3, 2, 5)),
            dma((4,)),
            dma((4,)),
            dma((2, 2)),
            dma((2, 2)),
            dma((2,)),
            dma((2,)),
            dma((7,)),
            dma((7,)),
            dma((15,)),
            dma((15,)),
            pltpu.SemaphoreType.REGULAR,
            pltpu.SemaphoreType.REGULAR,
        ],
        compiler_params=pltpu.CompilerParams(
            collective_id=0, has_side_effects=True, vmem_limit_bytes=48 << 20
        ),
        name="probe_step",
    )(
        *(
            pltpu.with_memory_space_constraint(v, pltpu.MemorySpace.HBM)
            for v in (
                activations.reshape(tok, depth),
                labels.reshape(tok // 128, 128),
                weights.reshape(lines, 128),
            )
        )
    )
    held = [v.reshape(lines, 128) for v in (weights, first_moment, second_moment)]
    grad, weights, first_moment, second_moment = lax.optimization_barrier((grad, *held))
    clipped = factor * grad
    new_first = 0.9 * first_moment + 0.1 * clipped
    new_second = 0.999 * second_moment + 0.001 * clipped * clipped
    new_weights = weights - 0.001 * (new_first / (1.0 - 0.9**STEP)) / (
        jnp.sqrt(new_second / (1.0 - 0.999**STEP)) + 1e-08
    )
    outs = (v.reshape(rows, 1, width) for v in (new_weights, new_first, new_second))
    return (*outs, loss[0, 0])


def solution(mesh):
    rows = P("dp", "layer", None)
    return jax.shard_map(
        shards,
        mesh=mesh,
        in_specs=(rows, P("dp"), rows, rows, rows),
        out_specs=(rows, rows, rows, P()),
        check_vma=False,
    )
```

```python
import jax
import jax.numpy as jnp
from jax import lax
from jax.experimental import pallas as pl
from jax.experimental.pallas import tpu as pltpu
from jax.sharding import PartitionSpec as P

STEP = 10
BF16 = jnp.bfloat16
F32 = jnp.float32
MESH = pl.DeviceIdType.MESH


def kernel(
    tokens,
    a_hbm,
    labels_hbm,
    w_hbm,
    grad_ref,
    factor_ref,
    loss_ref,
    a_v,
    labels_ref,
    w32,
    wbuf,
    a_far,
    slopes,
    acc,
    part,
    sbuf,
    rbuf,
    sscale,
    rscale,
    slots1,
    slots2,
    ld_sem,
    ws_sem,
    wr_sem,
    ds_sem,
    dr_sem,
    as_sem,
    ar_sem,
    ss_sem,
    sr_sem,
    ms_sem,
    mr_sem,
    p1s,
    p1r,
    p2s,
    p2r,
    mid1,
    mid2,
):
    tok = a_v.shape[0]
    width = wbuf.shape[1]
    rows = wbuf.shape[0] // 16
    quarter = rows // 4
    chip = 2 * rows
    d = lax.axis_index("dp")
    lay = lax.axis_index("layer")
    x = d // 8
    y = (d // 2) % 4
    c = d % 2

    def dp_of(dx, dy, dc=0):
        return ((x + dx) % 2) * 8 + ((y + dy) % 4) * 2 + (c + dc) % 2

    load_a = pltpu.make_async_copy(a_hbm, a_v, ld_sem.at[0])
    load_w = pltpu.make_async_copy(w_hbm, w32, ld_sem.at[1])
    load_labels = pltpu.make_async_copy(labels_hbm, labels_ref, ld_sem.at[2])
    load_w.start()
    load_a.start()
    load_labels.start()

    away = (lay + 4) % 8
    z_next, z_last = (lay // 4 * 4 + (lay + k) % 4 for k in (1, 3))
    near = [
        {"dp": dp_of(1, 0)},
        {"dp": dp_of(1, 0), "layer": away},
        {"dp": dp_of(0, 1)},
        {"dp": dp_of(0, 3)},
        {"dp": dp_of(0, 0, 1)},
        {"layer": z_next},
        {"layer": z_last},
    ]
    barrier = pltpu.get_barrier_semaphore()
    for who in near:
        pl.semaphore_signal(barrier, inc=1, device_id=who, device_id_type=MESH)

    with jax.named_scope("start"):
        load_w.wait()
        own = pl.multiple_of(d * rows, 64)

        def convert(g, carry):
            for j in range(4):
                v = w32[pl.ds(g * 64 + j, 16, stride=4), :]
                wbuf[pl.ds(pl.multiple_of(own + g * 16, 16), 16), j * 128 : (j + 1) * 128] = v.astype(BF16)
            return carry

        lax.fori_loop(0, rows // 16, convert, 0)
        with jax.named_scope("barrier"):
            pl.semaphore_wait(barrier, len(near))

    sent = []

    def copy_of(src, dst, ssem, rsem, dp):
        return pltpu.make_async_remote_copy(
            src_ref=src, dst_ref=dst, send_sem=ssem, recv_sem=rsem,
            device_id={"dp": dp}, device_id_type=MESH,
        )

    def send(*what):
        cp = copy_of(*what)
        cp.start()
        sent.append(cp)

    def arrived(ref, rsem):
        copy_of(ref, ref, ws_sem.at[0], rsem, dp_of(0, 0, 1)).wait_recv()

    def w_rows(dx, dy, dc, q):
        start = pl.multiple_of(dp_of(dx, dy, dc) * rows + q * quarter, 16)
        return wbuf.at[pl.ds(start, quarter), :]

    wcount = [0]

    def w_send(dx, dy, q, *targets):
        ref = w_rows(dx, dy, 0, q)
        for tx, ty in targets:
            k = ((dx - tx) % 2) * 4 + (dy - ty) % 4
            send(ref, ref, ws_sem.at[wcount[0]], wr_sem.at[k, q], dp_of(tx, ty))
            wcount[0] += 1

    def w_pass(dx, dy, q):
        ref = w_rows(dx, dy, 0, q)
        k = dx * 4 + dy
        send(ref, ref, ds_sem.at[k, q], dr_sem.at[k, q], dp_of(0, 0, 1))

    def w_take(dx, dy, q, *targets):
        arrived(w_rows(dx, dy, 0, q), wr_sem.at[dx * 4 + dy, q])
        w_send(dx, dy, q, *targets)
        w_pass(dx, dy, q)

    def chip_cols(dx, dy):
        return pl.multiple_of((((x + dx) % 2) * 4 + (y + dy) % 4) * chip, 128)

    acc[...] = jnp.zeros_like(acc)

    def logits_of(dx, dy):
        cols = chip_cols(dx, dy)
        for q in range(4):
            arrived(w_rows(dx, dy, 1, q), dr_sem.at[dx * 4 + dy, q])

        def step(n, carry):
            lanes = pl.ds(pl.multiple_of(n * 256, 256), 256)
            acc[:, lanes] += jnp.dot(
                a_v[:, pl.ds(cols, chip)], wbuf[pl.ds(cols, chip), lanes],
                preferred_element_type=F32,
            )
            return carry

        lax.fori_loop(0, width // 256, step, 0)

    X, UP, DOWN = (1, 0), (0, 1), (0, 3)
    for who in near[-2:]:
        pl.semaphore_signal(mid1, inc=1, device_id=who, device_id_type=MESH)
    with jax.named_scope("own"):
        for dest, q in (
            (X, 0), (UP, 2), (DOWN, 3), (X, 1), (UP, 3), (DOWN, 2),
            (X, 2), (UP, 0), (DOWN, 1), (X, 3), (UP, 1), (DOWN, 0),
        ):
            w_send(0, 0, q, dest)
        for q in range(4):
            w_pass(0, 0, q)
        for k in range(8):
            start = pl.multiple_of(k * chip + (1 - c) * 384, 128)
            send(
                a_hbm.at[:, pl.ds(start, 512)], a_far.at[k], as_sem.at[k], ar_sem.at[k],
                dp_of(0, 0, 1),
            )
        load_a.wait()
        load_labels.wait()

    with jax.named_scope("relay1"):
        w_take(0, 3, 2, UP, X)
        w_take(0, 1, 3, DOWN, X)
        w_take(0, 3, 3, X)
        w_take(0, 1, 2, X)
        w_take(1, 0, 0, UP, DOWN)
        w_take(1, 0, 1, UP, DOWN)
    with jax.named_scope("relay2"):
        logits_of(0, 0)
        w_take(0, 3, 0, UP)
        w_take(0, 1, 1, DOWN)
        w_take(0, 3, 1)
        w_take(0, 1, 0)
        w_take(1, 0, 2)
        w_take(1, 0, 3)
    with jax.named_scope("relay3"):
        w_take(0, 2, 2, X)
        w_take(0, 2, 3, X)
        logits_of(1, 0)
        logits_of(0, 3)
        logits_of(0, 1)
    with jax.named_scope("relay4"):
        w_take(1, 3, 0, UP)
        w_take(1, 1, 1, DOWN)
        w_take(1, 3, 1)
        w_take(1, 1, 0)
    with jax.named_scope("relay5"):
        for q in (2, 3):
            w_take(1, 3, q)
            w_take(1, 1, q)
        w_take(0, 2, 0)
        w_take(0, 2, 1)
        logits_of(0, 2)
        logits_of(1, 3)
        logits_of(1, 1)
    with jax.named_scope("relay6"):
        for q in range(4):
            w_take(1, 2, q)
        logits_of(1, 2)

    with jax.named_scope("softmax"):
        classes = lax.broadcasted_iota(jnp.int32, (128, width), 1)
        loss_lanes = jnp.zeros((1, 128), F32)
        for t in range(tok // 128):
            lab = jnp.broadcast_to(labels_ref[t : t + 1, :], (128, 128)).T
            lab = jnp.concatenate([lab] * (width // 128), axis=1)
            logits = acc[t * 128 : (t + 1) * 128, :]
            top = jnp.max(logits, axis=1, keepdims=True)
            exps = jnp.exp(logits - top)
            denom = jnp.sum(exps, axis=1, keepdims=True)
            onehot = (lab == classes).astype(F32)
            picked = jnp.sum(logits * onehot, axis=1, keepdims=True)
            probs = exps / denom
            slopes[0, t * 128 : (t + 1) * 128, :] = ((probs - onehot) / tokens).astype(BF16)
            term = top + jnp.log(denom) - picked
            loss_lanes += jnp.sum(jnp.broadcast_to(term, (128, 128)), axis=0, keepdims=True)

    send(slopes.at[0], slopes.at[1], ss_sem.at[0], sr_sem.at[0], dp_of(0, 0, 1))
    pl.semaphore_wait(mid1, 2)
    pl.semaphore_signal(mid2, inc=1, device_id={"layer": away}, device_id_type=MESH)

    def outer(left, right):
        return lax.dot_general(
            left, right, (((0,), (0,)), ((), ())), preferred_element_type=F32
        )

    def near_tokens(k, carry):
        cols = pl.multiple_of(k * chip + c * 384, 128)
        part[k] = outer(a_v[:, pl.ds(cols, 512)], slopes[0])
        return carry

    with jax.named_scope("own_tokens"):
        lax.fori_loop(0, 8, near_tokens, 0)
    with jax.named_scope("partner"):
        for k in range(8):
            arrived(a_far.at[k], ar_sem.at[k])
        arrived(slopes.at[1], sr_sem.at[0])

    def at(dx, dy):
        return ((x + dx) % 2) * 4 + (y + dy) % 4

    def far_tokens(dx, dy):
        k = at(dx, dy)
        part[k] += outer(a_far[k], slopes[1])

    def partial(dx, dy, q):
        return part[at(dx, dy), pl.ds(pl.multiple_of(c * 64 + q * quarter, 16), quarter), :]

    def ship(i, value, dest):
        top = jnp.maximum(jnp.max(jnp.abs(value), axis=0, keepdims=True), 1e-30)
        sbuf[i] = jnp.round(value * (32767.0 / top)).astype(jnp.int32).astype(jnp.int16)
        sscale[i] = top * (1.0 / 32767.0)
        send(sbuf.at[i], rbuf.at[i], ms_sem.at[i, 0], mr_sem.at[i, 0], dp_of(*dest))
        send(sscale.at[i], rscale.at[i], ms_sem.at[i, 1], mr_sem.at[i, 1], dp_of(*dest))

    def got(i):
        arrived(rbuf.at[i], mr_sem.at[i, 0])
        arrived(rscale.at[i], mr_sem.at[i, 1])
        return rbuf[i].astype(jnp.int32).astype(F32) * rscale[i]

    def x_first(dy, q):
        return dy * 2 + q

    def x_last(q):
        return 8 + q - 2

    def base(side):
        return 10 if side == UP else 19

    def two(side, kind):
        return base(side) + kind

    def one(side, kind, q):
        return base(side) + 3 + kind * 2 + q % 2

    with jax.named_scope("rs_a"):
        far_tokens(1, 2)
        ship(two(UP, 1), partial(1, 2, 2), UP)
        ship(two(DOWN, 1), partial(1, 2, 3), DOWN)
        for q in (0, 1):
            ship(x_first(2, q), partial(1, 2, q), X)
        far_tokens(0, 2)
        ship(two(UP, 0), partial(0, 2, 2), UP)
        ship(two(DOWN, 0), partial(0, 2, 3), DOWN)
    with jax.named_scope("rs_b"):
        far_tokens(1, 1)
        ship(one(UP, 1, 3), partial(1, 1, 3), UP)
        far_tokens(1, 3)
        ship(one(DOWN, 1, 2), partial(1, 3, 2), DOWN)
        ship(x_first(1, 1), partial(1, 1, 1), X)
        ship(x_first(3, 0), partial(1, 3, 0), X)
        far_tokens(0, 1)
        ship(one(UP, 0, 3), partial(0, 1, 3), UP)
        far_tokens(0, 3)
        ship(one(DOWN, 0, 2), partial(0, 3, 2), DOWN)
        ship(x_first(1, 0), partial(1, 1, 0), X)
        ship(x_first(3, 1), partial(1, 3, 1), X)
        far_tokens(1, 0)
        for q in (0, 1):
            ship(x_first(0, q), partial(1, 0, q), X)
        far_tokens(0, 0)
    with jax.named_scope("rs_c"):
        for kind in (1, 0):
            ship(one(UP, kind, 2), partial(kind, 1, 2) + got(two(UP, kind)), UP)
            ship(one(DOWN, kind, 3), partial(kind, 3, 3) + got(two(DOWN, kind)), DOWN)
    with jax.named_scope("rs_d"):
        ship(two(UP, 2), partial(0, 2, 0) + got(x_first(2, 0)), UP)
        ship(two(DOWN, 2), partial(0, 2, 1) + got(x_first(2, 1)), DOWN)
    with jax.named_scope("rs_e"):
        ship(one(UP, 2, 1), partial(0, 1, 1) + got(x_first(1, 1)), UP)
        ship(one(DOWN, 2, 0), partial(0, 3, 0) + got(x_first(3, 0)), DOWN)
    with jax.named_scope("rs_f"):
        pl.semaphore_wait(mid2, 1)
        for q in (3, 2):
            ship(x_last(q), partial(1, 0, q) + got(one(UP, 1, q)) + got(one(DOWN, 1, q)), X)
    with jax.named_scope("rs_g"):
        ship(one(UP, 2, 0), partial(0, 1, 0) + got(x_first(1, 0)) + got(two(UP, 2)), UP)
        ship(one(DOWN, 2, 1), partial(0, 3, 1) + got(x_first(3, 1)) + got(two(DOWN, 2)), DOWN)

    def finish(q, total, carry):
        for g in range(quarter // 8):
            for j in range(4):
                v = total[g * 8 : (g + 1) * 8, j * 128 : (j + 1) * 128]
                grad_ref[pl.ds((q * quarter + g * 8) * 4 + j, 8, stride=4), :] = v
                carry = carry + v * v
        return carry

    square = jnp.zeros((8, 128), F32)
    with jax.named_scope("fin_a"):
        for q in (3, 2):
            total = partial(0, 0, q) + got(one(UP, 0, q)) + got(one(DOWN, 0, q))
            part[at(0, 0), pl.ds(pl.multiple_of(c * 64 + q * quarter, 16), quarter), :] = total
        for q in (0, 1):
            total = partial(0, 0, q) + got(x_first(0, q))
            part[at(0, 0), pl.ds(pl.multiple_of(c * 64 + q * quarter, 16), quarter), :] = total
    with jax.named_scope("fin_b"):
        for q in (1, 0):
            total = partial(0, 0, q) + got(one(UP, 2, q)) + got(one(DOWN, 2, q))
            square = finish(q, total, square)
    with jax.named_scope("fin_c"):
        for q in (3, 2):
            square = finish(q, partial(0, 0, q) + got(x_last(q)), square)
        tile = jnp.concatenate(
            [jnp.sum(square, axis=0, keepdims=True), loss_lanes, jnp.zeros((6, 128), F32)], axis=0
        )

    def spread(slots, here, index, peers, ssem, rsem):
        slots[index] = here
        copies = []
        for k, who in enumerate(peers):
            cp = pltpu.make_async_remote_copy(
                src_ref=slots.at[index], dst_ref=slots.at[index], send_sem=ssem.at[k],
                recv_sem=rsem.at[k], device_id=who, device_id_type=MESH,
            )
            cp.start()
            copies.append(cp)
        while sent:
            sent.pop().wait_send()
        for cp in copies:
            cp.wait()
        return jnp.sum(slots[...], axis=0)

    m = y * 2 + c
    n = x * 8 + lay
    with jax.named_scope("red1"):
        tile = spread(
            slots1, tile, m, [{"dp": x * 8 + (m + k) % 8} for k in range(1, 8)], p1s, p1r
        )
    with jax.named_scope("red2"):
        others = [(n + k) % 16 for k in range(1, 16)]
        sums = spread(
            slots2, tile, n, [{"dp": o // 8 * 8 + m, "layer": o % 8} for o in others], p2s, p2r
        )
    square = jnp.broadcast_to(jnp.sum(sums[0:1, :], axis=1, keepdims=True), (1, 128))
    factor_ref[...] = jnp.minimum(1.0, 0.25 / jnp.sqrt(square + 1e-12))
    loss_ref[...] = sums[1:2, :] / (tokens * 8)


def shards(activations, labels, weights, first_moment, second_moment):
    tok = activations.shape[0]
    depth = activations.shape[2]
    rows, _, width = weights.shape
    tokens = tok * lax.axis_size("dp")
    dma = pltpu.SemaphoreType.DMA
    vmem = pltpu.VMEM
    lines = rows * width // 128
    anywhere = pl.BlockSpec(memory_space=pltpu.MemorySpace.HBM)
    inside = pl.BlockSpec(memory_space=pltpu.VMEM)

    def body(*refs):
        kernel(tokens, *refs)

    grad, factor, loss = pl.pallas_call(
        body,
        out_shape=(
            jax.ShapeDtypeStruct((lines, 128), F32),
            jax.ShapeDtypeStruct((1, 128), F32),
            jax.ShapeDtypeStruct((1, 128), F32),
        ),
        in_specs=[anywhere, anywhere, anywhere],
        out_specs=(inside, inside, inside),
        scratch_shapes=[
            vmem((tok, depth), BF16),
            vmem((tok // 128, 128), jnp.int32),
            vmem((lines, 128), F32),
            vmem((depth, width), BF16),
            vmem((8, tok, 512), BF16),
            vmem((2, tok, width), BF16),
            vmem((tok, width), F32),
            vmem((8, 512, width), F32),
            vmem((28, rows // 4, width), jnp.int16),
            vmem((28, rows // 4, width), jnp.int16),
            vmem((28, 1, width), F32),
            vmem((28, 1, width), F32),
            vmem((8, 8, 128), F32),
            vmem((16, 8, 128), F32),
            dma((3,)),
            dma((28,)),
            dma((8, 4)),
            dma((8, 4)),
            dma((8, 4)),
            dma((8,)),
            dma((8,)),
            dma((1,)),
            dma((1,)),
            dma((28, 2)),
            dma((28, 2)),
            dma((7,)),
            dma((7,)),
            dma((15,)),
            dma((15,)),
            pltpu.SemaphoreType.REGULAR,
            pltpu.SemaphoreType.REGULAR,
        ],
        compiler_params=pltpu.CompilerParams(
            collective_id=0, has_side_effects=True, vmem_limit_bytes=48 << 20
        ),
        name="probe_step",
    )(
        *(
            pltpu.with_memory_space_constraint(v, pltpu.MemorySpace.HBM)
            for v in (
                activations.reshape(tok, depth),
                labels.reshape(tok // 128, 128),
                weights.reshape(lines, 128),
            )
        )
    )
    held = [v.reshape(lines, 128) for v in (weights, first_moment, second_moment)]
    grad, weights, first_moment, second_moment = lax.optimization_barrier((grad, *held))
    clipped = factor * grad
    new_first = 0.9 * first_moment + 0.1 * clipped
    new_second = 0.999 * second_moment + 0.001 * clipped * clipped
    new_weights = weights - 0.001 * (new_first / (1.0 - 0.9**STEP)) / (
        jnp.sqrt(new_second / (1.0 - 0.999**STEP)) + 1e-08
    )
    outs = (v.reshape(rows, 1, width) for v in (new_weights, new_first, new_second))
    return (*outs, loss[0, 0])


def solution(mesh):
    rows = P("dp", "layer", None)
    return jax.shard_map(
        shards,
        mesh=mesh,
        in_specs=(rows, P("dp"), rows, rows, rows),
        out_specs=(rows, rows, rows, P()),
        check_vma=False,
    )
```

```python
import jax
import jax.numpy as jnp
from jax import lax
from jax.experimental import pallas as pl
from jax.experimental.pallas import tpu as pltpu
from jax.sharding import PartitionSpec as P

STEP = 10
BF16 = jnp.bfloat16
F32 = jnp.float32
MESH = pl.DeviceIdType.MESH


def kernel(
    tokens,
    a_hbm,
    labels_hbm,
    w_hbm,
    grad_ref,
    factor_ref,
    loss_ref,
    a_v,
    labels_ref,
    w32,
    grad_v,
    wbuf,
    a_far,
    slopes,
    acc,
    part,
    sbuf,
    rbuf,
    sscale,
    rscale,
    slots1,
    slots2,
    ld_sem,
    sent_sem,
    wr_sem,
    dr_sem,
    ar_sem,
    sr_sem,
    mr_sem,
    red_sem,
    mid1,
    mid2,
):
    tok = a_v.shape[0]
    width = wbuf.shape[1]
    rows = wbuf.shape[0] // 16
    starts, sizes = (0, 96, 192, 320), (96, 96, 128, 128)
    w_starts, w_sizes = (0, 128, 256, 352), (128, 128, 96, 96)
    chip = 2 * rows
    d = lax.axis_index("dp")
    lay = lax.axis_index("layer")
    x = d // 8
    y = (d // 2) % 4
    c = d % 2

    def dp_of(dx, dy, dc=0):
        return ((x + dx) % 2) * 8 + ((y + dy) % 4) * 2 + (c + dc) % 2

    load_a = pltpu.make_async_copy(a_hbm, a_v, ld_sem.at[0])
    load_w = pltpu.make_async_copy(w_hbm, w32, ld_sem.at[1])
    load_labels = pltpu.make_async_copy(labels_hbm, labels_ref, ld_sem.at[2])
    load_w.start()
    load_a.start()
    load_labels.start()

    away = (lay + 4) % 8
    z_next, z_last = (lay // 4 * 4 + (lay + k) % 4 for k in (1, 3))
    near = [
        {"dp": dp_of(1, 0)},
        {"dp": dp_of(1, 0), "layer": away},
        {"dp": dp_of(0, 1)},
        {"dp": dp_of(0, 3)},
        {"dp": dp_of(0, 0, 1)},
        {"layer": z_next},
        {"layer": z_last},
    ]
    barrier = pltpu.get_barrier_semaphore()
    for who in near:
        pl.semaphore_signal(barrier, inc=1, device_id=who, device_id_type=MESH)

    with jax.named_scope("start"):
        load_w.wait()
        own = pl.multiple_of(d * rows, 64)

        def convert(g, carry):
            for j in range(4):
                v = w32[pl.ds(g * 64 + j, 16, stride=4), :]
                wbuf[pl.ds(pl.multiple_of(own + g * 16, 16), 16), j * 128 : (j + 1) * 128] = v.astype(BF16)
            return carry

        lax.fori_loop(0, rows // 16, convert, 0)
        with jax.named_scope("barrier"):
            pl.semaphore_wait(barrier, len(near))


    def copy_of(src, dst, ssem, rsem, dp):
        return pltpu.make_async_remote_copy(
            src_ref=src, dst_ref=dst, send_sem=ssem, recv_sem=rsem,
            device_id={"dp": dp}, device_id_type=MESH,
        )

    def send(family, src, dst, rsem, dp):
        copy_of(src, dst, sent_sem.at[family], rsem, dp).start()

    def all_sent(family, like):
        copy_of(like, like, sent_sem.at[family], sent_sem.at[family], dp_of(0, 0, 1)).wait_send()

    def arrived(ref, rsem):
        copy_of(ref, ref, sent_sem.at[0], rsem, dp_of(0, 0, 1)).wait_recv()

    def w_rows(dx, dy, dc, q):
        start = pl.multiple_of(dp_of(dx, dy, dc) * rows + w_starts[q], 32)
        return wbuf.at[pl.ds(start, w_sizes[q]), :]

    def w_send(dx, dy, q, *targets):
        ref = w_rows(dx, dy, 0, q)
        for tx, ty in targets:
            k = ((dx - tx) % 2) * 4 + (dy - ty) % 4
            send(0, ref, ref, wr_sem.at[k, q], dp_of(tx, ty))

    def w_pass(dx, dy, q):
        ref = w_rows(dx, dy, 0, q)
        k = dx * 4 + dy
        send(1, ref, ref, dr_sem.at[k], dp_of(0, 0, 1))

    def w_take(dx, dy, q, *targets):
        arrived(w_rows(dx, dy, 0, q), wr_sem.at[dx * 4 + dy, q])
        w_send(dx, dy, q, *targets)
        w_pass(dx, dy, q)

    def chip_cols(dx, dy):
        return pl.multiple_of((((x + dx) % 2) * 4 + (y + dy) % 4) * chip, 128)

    acc[...] = jnp.zeros_like(acc)

    def logits_of(dx, dy):
        cols = chip_cols(dx, dy)
        start = pl.multiple_of(dp_of(dx, dy, 1) * rows, 32)
        arrived(wbuf.at[pl.ds(start, rows), :], dr_sem.at[dx * 4 + dy])

        def step(n, carry):
            lanes = pl.ds(pl.multiple_of(n * 256, 256), 256)
            acc[:, lanes] += jnp.dot(
                a_v[:, pl.ds(cols, chip)], wbuf[pl.ds(cols, chip), lanes],
                preferred_element_type=F32,
            )
            return carry

        lax.fori_loop(0, width // 256, step, 0)

    X, UP, DOWN = (1, 0), (0, 1), (0, 3)
    for who in near[-2:]:
        pl.semaphore_signal(mid1, inc=1, device_id=who, device_id_type=MESH)
    with jax.named_scope("own"):
        for dest, q in (
            (X, 0), (UP, 2), (DOWN, 3), (X, 1), (UP, 3), (DOWN, 2),
            (X, 2), (UP, 0), (DOWN, 1), (X, 3), (UP, 1), (DOWN, 0),
        ):
            w_send(0, 0, q, dest)
        for q in range(4):
            w_pass(0, 0, q)
        for k in range(8):
            start = pl.multiple_of(k * chip + (1 - c) * 384, 128)
            send(2, a_hbm.at[:, pl.ds(start, 512)], a_far.at[k], ar_sem.at[0], dp_of(0, 0, 1))
        load_a.wait()
        load_labels.wait()

    with jax.named_scope("relay1"):
        w_take(0, 3, 2, UP, X)
        w_take(0, 1, 3, DOWN, X)
        w_take(0, 3, 3, X)
        w_take(0, 1, 2, X)
        w_take(1, 0, 0, UP, DOWN)
        w_take(1, 0, 1, UP, DOWN)
    with jax.named_scope("relay2"):
        logits_of(0, 0)
        w_take(0, 3, 0, UP)
        w_take(0, 1, 1, DOWN)
        w_take(0, 3, 1)
        w_take(0, 1, 0)
        w_take(1, 0, 2)
        w_take(1, 0, 3)
    with jax.named_scope("relay3"):
        w_take(0, 2, 2, X)
        w_take(0, 2, 3, X)
        logits_of(1, 0)
        logits_of(0, 3)
        logits_of(0, 1)
    with jax.named_scope("relay4"):
        w_take(1, 3, 0, UP)
        w_take(1, 1, 1, DOWN)
        w_take(1, 3, 1)
        w_take(1, 1, 0)
    with jax.named_scope("relay5"):
        for q in (2, 3):
            w_take(1, 3, q)
            w_take(1, 1, q)
        w_take(0, 2, 0)
        w_take(0, 2, 1)
        logits_of(0, 2)
        logits_of(1, 3)
        logits_of(1, 1)
    with jax.named_scope("relay6"):
        for q in range(4):
            w_take(1, 2, q)
        logits_of(1, 2)

    with jax.named_scope("softmax"):
        classes = lax.broadcasted_iota(jnp.int32, (128, width), 1)
        loss_lanes = jnp.zeros((1, 128), F32)
        for t in range(tok // 128):
            lab = jnp.broadcast_to(labels_ref[t : t + 1, :], (128, 128)).T
            lab = jnp.concatenate([lab] * (width // 128), axis=1)
            logits = acc[t * 128 : (t + 1) * 128, :]
            top = jnp.max(logits, axis=1, keepdims=True)
            exps = jnp.exp(logits - top)
            denom = jnp.sum(exps, axis=1, keepdims=True)
            onehot = (lab == classes).astype(F32)
            picked = jnp.sum(logits * onehot, axis=1, keepdims=True)
            probs = exps / denom
            slopes[0, t * 128 : (t + 1) * 128, :] = ((probs - onehot) / tokens).astype(BF16)
            term = top + jnp.log(denom) - picked
            loss_lanes += jnp.sum(jnp.broadcast_to(term, (128, 128)), axis=0, keepdims=True)

    send(3, slopes.at[0], slopes.at[1], sr_sem.at[0], dp_of(0, 0, 1))
    pl.semaphore_wait(mid1, 2)
    pl.semaphore_signal(mid2, inc=1, device_id={"layer": away}, device_id_type=MESH)

    def outer(left, right):
        return lax.dot_general(
            left, right, (((0,), (0,)), ((), ())), preferred_element_type=F32
        )

    def near_tokens(k, carry):
        cols = pl.multiple_of(k * chip + c * 384, 128)
        part[k] = outer(a_v[:, pl.ds(cols, 512)], slopes[0])
        return carry

    def at(dx, dy):
        return ((x + dx) % 2) * 4 + (y + dy) % 4

    ahead = ((1, 2), (0, 2), (1, 1), (1, 3))

    def tokens_of(dx, dy):
        k = at(dx, dy)
        if (dx, dy) not in ahead:
            near_tokens(k, 0)
        part[k] += outer(a_far[k], slopes[1])

    with jax.named_scope("own_tokens"):
        for who in ahead:
            near_tokens(at(*who), 0)
    with jax.named_scope("partner"):
        arrived(a_far, ar_sem.at[0])
        arrived(slopes.at[1], sr_sem.at[0])

    def block_rows(q):
        return pl.ds(pl.multiple_of(c * 64 + starts[q], 32), sizes[q])

    def partial(dx, dy, q):
        return part[at(dx, dy), block_rows(q), :]

    def ship(i, value, dest):
        top = jnp.maximum(jnp.max(jnp.abs(value), axis=0, keepdims=True), 1e-30)
        held = pl.ds(0, value.shape[0])
        sbuf[i, held, :] = jnp.round(value * (32767.0 / top)).astype(jnp.int32).astype(jnp.int16)
        sscale[i] = top * (1.0 / 32767.0)
        send(4, sbuf.at[i, held, :], rbuf.at[i, held, :], mr_sem.at[i, 0], dp_of(*dest))
        send(5, sscale.at[i], rscale.at[i], mr_sem.at[i, 1], dp_of(*dest))

    def got(i, q):
        held = pl.ds(0, sizes[q])
        arrived(rbuf.at[i, held, :], mr_sem.at[i, 0])
        arrived(rscale.at[i], mr_sem.at[i, 1])
        return rbuf[i, held, :].astype(jnp.int32).astype(F32) * rscale[i]

    def x_first(dy, q):
        return dy * 2 + q

    def x_last(q):
        return 8 + q - 2

    def base(side):
        return 10 if side == UP else 19

    def two(side, kind):
        return base(side) + kind

    def one(side, kind, q):
        return base(side) + 3 + kind * 2 + q % 2

    with jax.named_scope("rs_a"):
        tokens_of(1, 2)
        ship(two(UP, 1), partial(1, 2, 2), UP)
        ship(two(DOWN, 1), partial(1, 2, 3), DOWN)
        for q in (0, 1):
            ship(x_first(2, q), partial(1, 2, q), X)
        tokens_of(0, 2)
        ship(two(UP, 0), partial(0, 2, 2), UP)
        ship(two(DOWN, 0), partial(0, 2, 3), DOWN)
    with jax.named_scope("rs_b"):
        tokens_of(1, 1)
        ship(x_first(1, 1), partial(1, 1, 1), X)
        ship(one(UP, 1, 3), partial(1, 1, 3), UP)
        tokens_of(1, 3)
        ship(x_first(3, 0), partial(1, 3, 0), X)
        ship(one(DOWN, 1, 2), partial(1, 3, 2), DOWN)
        tokens_of(0, 1)
        ship(one(UP, 0, 3), partial(0, 1, 3), UP)
        tokens_of(0, 3)
        ship(one(DOWN, 0, 2), partial(0, 3, 2), DOWN)
        ship(x_first(1, 0), partial(1, 1, 0), X)
        ship(x_first(3, 1), partial(1, 3, 1), X)
        tokens_of(1, 0)
        for q in (0, 1):
            ship(x_first(0, q), partial(1, 0, q), X)
        tokens_of(0, 0)
    with jax.named_scope("rs_c"):
        for kind in (1, 0):
            ship(one(UP, kind, 2), partial(kind, 1, 2) + got(two(UP, kind), 2), UP)
            ship(one(DOWN, kind, 3), partial(kind, 3, 3) + got(two(DOWN, kind), 3), DOWN)
    with jax.named_scope("rs_d"):
        ship(two(UP, 2), partial(0, 2, 0) + got(x_first(2, 0), 0), UP)
        ship(two(DOWN, 2), partial(0, 2, 1) + got(x_first(2, 1), 1), DOWN)
    with jax.named_scope("rs_e"):
        ship(one(UP, 2, 1), partial(0, 1, 1) + got(x_first(1, 1), 1), UP)
        ship(one(DOWN, 2, 0), partial(0, 3, 0) + got(x_first(3, 0), 0), DOWN)
    with jax.named_scope("rs_f"):
        pl.semaphore_wait(mid2, 1)
        for q in (3, 2):
            ship(x_last(q), partial(1, 0, q) + got(one(UP, 1, q), q) + got(one(DOWN, 1, q), q), X)
    with jax.named_scope("rs_g"):
        ship(one(UP, 2, 0), partial(0, 1, 0) + got(x_first(1, 0), 0) + got(two(UP, 2), 0), UP)
        ship(one(DOWN, 2, 1), partial(0, 3, 1) + got(x_first(3, 1), 1) + got(two(DOWN, 2), 1), DOWN)

    def finish(q, total, carry):
        for g in range(sizes[q] // 8):
            for j in range(4):
                v = total[g * 8 : (g + 1) * 8, j * 128 : (j + 1) * 128]
                grad_v[pl.ds((starts[q] + g * 8) * 4 + j, 8, stride=4), :] = v
                carry = carry + v * v
        return carry

    square = jnp.zeros((8, 128), F32)
    with jax.named_scope("fin_a"):
        for q in (3, 2):
            total = partial(0, 0, q) + got(one(UP, 0, q), q) + got(one(DOWN, 0, q), q)
            part[at(0, 0), block_rows(q), :] = total
        for q in (0, 1):
            part[at(0, 0), block_rows(q), :] = partial(0, 0, q) + got(x_first(0, q), q)
    with jax.named_scope("fin_b"):
        for q in (1, 0):
            total = partial(0, 0, q) + got(one(UP, 2, q), q) + got(one(DOWN, 2, q), q)
            square = finish(q, total, square)
    with jax.named_scope("fin_c"):
        for q in (3, 2):
            square = finish(q, partial(0, 0, q) + got(x_last(q), q), square)
        tile = jnp.concatenate(
            [jnp.sum(square, axis=0, keepdims=True), loss_lanes, jnp.zeros((6, 128), F32)], axis=0
        )
        store = pltpu.make_async_copy(grad_v, grad_ref, ld_sem.at[3])
        store.start()

    def spread(slots, here, index, peers, stage):
        slots[index] = here
        for who in peers:
            pltpu.make_async_remote_copy(
                src_ref=slots.at[index], dst_ref=slots.at[index], send_sem=sent_sem.at[6 + stage],
                recv_sem=red_sem.at[stage], device_id=who, device_id_type=MESH,
            ).start()
        if stage == 0:
            moved = 7 * rows
            all_sent(0, wbuf.at[pl.ds(0, moved), :])
            all_sent(1, wbuf.at[pl.ds(0, 8 * rows), :])
            all_sent(2, a_far)
            all_sent(3, slopes.at[0])
            all_sent(4, wbuf.at[pl.ds(0, moved), :])
            all_sent(5, sscale)
        some = slots.at[pl.ds(0, len(peers))]
        arrived(some, red_sem.at[stage])
        all_sent(6 + stage, some)
        return jnp.sum(slots[...], axis=0)

    m = y * 2 + c
    n = x * 8 + lay
    with jax.named_scope("red1"):
        tile = spread(
            slots1, tile, m, [{"dp": x * 8 + (m + k) % 8} for k in range(1, 8)], 0
        )
    with jax.named_scope("red2"):
        others = [(n + k) % 16 for k in range(1, 16)]
        sums = spread(
            slots2, tile, n, [{"dp": o // 8 * 8 + m, "layer": o % 8} for o in others], 1
        )
    with jax.named_scope("end1"):
        store.wait()
    square = jnp.broadcast_to(jnp.sum(sums[0:1, :], axis=1, keepdims=True), (1, 128))
    factor_ref[...] = jnp.minimum(1.0, 0.25 / jnp.sqrt(square + 1e-12))
    loss_ref[...] = sums[1:2, :] / (tokens * 8)


def shards(activations, labels, weights, first_moment, second_moment):
    tok = activations.shape[0]
    depth = activations.shape[2]
    rows, _, width = weights.shape
    tokens = tok * lax.axis_size("dp")
    dma = pltpu.SemaphoreType.DMA
    vmem = pltpu.VMEM
    lines = rows * width // 128
    anywhere = pl.BlockSpec(memory_space=pltpu.MemorySpace.HBM)
    inside = pl.BlockSpec(memory_space=pltpu.VMEM)

    def body(*refs):
        kernel(tokens, *refs)

    grad, factor, loss = pl.pallas_call(
        body,
        out_shape=(
            jax.ShapeDtypeStruct((lines, 128), F32),
            jax.ShapeDtypeStruct((1, 128), F32),
            jax.ShapeDtypeStruct((1, 128), F32),
        ),
        in_specs=[anywhere, anywhere, anywhere],
        out_specs=(anywhere, inside, inside),
        scratch_shapes=[
            vmem((tok, depth), BF16),
            vmem((tok // 128, 128), jnp.int32),
            vmem((lines, 128), F32),
            vmem((lines, 128), F32),
            vmem((depth, width), BF16),
            vmem((8, tok, 512), BF16),
            vmem((2, tok, width), BF16),
            vmem((tok, width), F32),
            vmem((8, 512, width), F32),
            vmem((28, 128, width), jnp.int16),
            vmem((28, 128, width), jnp.int16),
            vmem((28, 1, width), F32),
            vmem((28, 1, width), F32),
            vmem((8, 8, 128), F32),
            vmem((16, 8, 128), F32),
            dma((4,)),
            dma((8,)),
            dma((8, 4)),
            dma((8,)),
            dma((1,)),
            dma((1,)),
            dma((28, 2)),
            dma((2,)),
            pltpu.SemaphoreType.REGULAR,
            pltpu.SemaphoreType.REGULAR,
        ],
        compiler_params=pltpu.CompilerParams(
            collective_id=0, has_side_effects=True, vmem_limit_bytes=48 << 20
        ),
        name="probe_step",
    )(
        *(
            pltpu.with_memory_space_constraint(v, pltpu.MemorySpace.HBM)
            for v in (
                activations.reshape(tok, depth),
                labels.reshape(tok // 128, 128),
                weights.reshape(lines, 128),
            )
        )
    )
    held = [v.reshape(lines, 128) for v in (weights, first_moment, second_moment)]
    grad, weights, first_moment, second_moment = lax.optimization_barrier((grad, *held))
    clipped = factor * grad
    new_first = 0.9 * first_moment + 0.1 * clipped
    new_second = 0.999 * second_moment + 0.001 * clipped * clipped
    new_weights = weights - 0.001 * (new_first / (1.0 - 0.9**STEP)) / (
        jnp.sqrt(new_second / (1.0 - 0.999**STEP)) + 1e-08
    )
    outs = (v.reshape(rows, 1, width) for v in (new_weights, new_first, new_second))
    return (*outs, loss[0, 0])


def solution(mesh):
    rows = P("dp", "layer", None)
    return jax.shard_map(
        shards,
        mesh=mesh,
        in_specs=(rows, P("dp"), rows, rows, rows),
        out_specs=(rows, rows, rows, P()),
        check_vma=False,
    )
```

```python
import jax
import jax.numpy as jnp
from jax import lax
from jax.experimental import pallas as pl
from jax.experimental.pallas import tpu as pltpu
from jax.sharding import PartitionSpec as P

STEP = 10
BF16 = jnp.bfloat16
F32 = jnp.float32
MESH = pl.DeviceIdType.MESH


def kernel(
    tokens,
    a_hbm,
    labels_hbm,
    w_hbm,
    grad_ref,
    factor_ref,
    loss_ref,
    a_v,
    labels_ref,
    w32,
    grad_v,
    wbuf,
    a_far,
    slopes,
    acc,
    part,
    sbuf,
    rbuf,
    sscale,
    rscale,
    slots1,
    slots2,
    ld_sem,
    sent_sem,
    wr_sem,
    dr_sem,
    ar_sem,
    sr_sem,
    mr_sem,
    red_sem,
    mid1,
    mid2,
):
    tok = a_v.shape[0]
    width = wbuf.shape[1]
    rows = wbuf.shape[0] // 16
    starts, sizes = (0, 96, 192, 320), (96, 96, 128, 128)
    w_starts, w_sizes = (0, 128, 256, 352), (128, 128, 96, 96)
    chip = 2 * rows
    d = lax.axis_index("dp")
    lay = lax.axis_index("layer")
    x = d // 8
    y = (d // 2) % 4
    c = d % 2

    def dp_of(dx, dy, dc=0):
        return ((x + dx) % 2) * 8 + ((y + dy) % 4) * 2 + (c + dc) % 2

    load_a = pltpu.make_async_copy(a_hbm, a_v, ld_sem.at[0])
    load_w = pltpu.make_async_copy(w_hbm, w32, ld_sem.at[1])
    load_labels = pltpu.make_async_copy(labels_hbm, labels_ref, ld_sem.at[2])
    load_w.start()
    load_a.start()
    load_labels.start()

    away = (lay + 4) % 8
    z_next, z_last = (lay // 4 * 4 + (lay + k) % 4 for k in (1, 3))
    near = [
        {"dp": dp_of(1, 0)},
        {"dp": dp_of(1, 0), "layer": away},
        {"dp": dp_of(0, 1)},
        {"dp": dp_of(0, 3)},
        {"dp": dp_of(0, 0, 1)},
        {"layer": z_next},
        {"layer": z_last},
    ]
    barrier = pltpu.get_barrier_semaphore()
    for who in near:
        pl.semaphore_signal(barrier, inc=1, device_id=who, device_id_type=MESH)

    with jax.named_scope("start"):
        load_w.wait()
        own = pl.multiple_of(d * rows, 64)

        def convert(g, carry):
            for j in range(4):
                v = w32[pl.ds(g * 64 + j, 16, stride=4), :]
                wbuf[pl.ds(pl.multiple_of(own + g * 16, 16), 16), j * 128 : (j + 1) * 128] = v.astype(BF16)
            return carry

        lax.fori_loop(0, rows // 16, convert, 0)
        with jax.named_scope("barrier"):
            pl.semaphore_wait(barrier, len(near))


    def copy_of(src, dst, ssem, rsem, dp):
        return pltpu.make_async_remote_copy(
            src_ref=src, dst_ref=dst, send_sem=ssem, recv_sem=rsem,
            device_id={"dp": dp}, device_id_type=MESH,
        )

    def send(family, src, dst, rsem, dp):
        copy_of(src, dst, sent_sem.at[family], rsem, dp).start()

    def all_sent(family, like):
        copy_of(like, like, sent_sem.at[family], sent_sem.at[family], dp_of(0, 0, 1)).wait_send()

    def arrived(ref, rsem):
        copy_of(ref, ref, sent_sem.at[0], rsem, dp_of(0, 0, 1)).wait_recv()

    def w_rows(dx, dy, dc, q):
        start = pl.multiple_of(dp_of(dx, dy, dc) * rows + w_starts[q], 32)
        return wbuf.at[pl.ds(start, w_sizes[q]), :]

    def w_send(dx, dy, q, *targets):
        ref = w_rows(dx, dy, 0, q)
        for tx, ty in targets:
            k = ((dx - tx) % 2) * 4 + (dy - ty) % 4
            send(0, ref, ref, wr_sem.at[k, q], dp_of(tx, ty))

    def w_pass(dx, dy, q):
        ref = w_rows(dx, dy, 0, q)
        k = dx * 4 + dy
        send(1, ref, ref, dr_sem.at[k], dp_of(0, 0, 1))

    def w_take(dx, dy, q, *targets):
        arrived(w_rows(dx, dy, 0, q), wr_sem.at[dx * 4 + dy, q])
        w_send(dx, dy, q, *targets)
        w_pass(dx, dy, q)

    def chip_cols(dx, dy):
        return pl.multiple_of((((x + dx) % 2) * 4 + (y + dy) % 4) * chip, 128)

    acc[...] = jnp.zeros_like(acc)

    def logits_of(dx, dy):
        cols = chip_cols(dx, dy)
        start = pl.multiple_of(dp_of(dx, dy, 1) * rows, 32)
        arrived(wbuf.at[pl.ds(start, rows), :], dr_sem.at[dx * 4 + dy])

        def step(n, carry):
            lanes = pl.ds(pl.multiple_of(n * 256, 256), 256)
            acc[:, lanes] += jnp.dot(
                a_v[:, pl.ds(cols, chip)], wbuf[pl.ds(cols, chip), lanes],
                preferred_element_type=F32,
            )
            return carry

        lax.fori_loop(0, width // 256, step, 0)

    X, UP, DOWN = (1, 0), (0, 1), (0, 3)
    for who in near[-2:]:
        pl.semaphore_signal(mid1, inc=1, device_id=who, device_id_type=MESH)
    with jax.named_scope("own"):
        for dest, q in (
            (X, 0), (UP, 2), (DOWN, 3), (X, 1), (UP, 3), (DOWN, 2),
            (X, 2), (UP, 0), (DOWN, 1), (X, 3), (UP, 1), (DOWN, 0),
        ):
            w_send(0, 0, q, dest)
        for q in range(4):
            w_pass(0, 0, q)
        for k in range(8):
            start = pl.multiple_of(k * chip + (1 - c) * 384, 128)
            send(2, a_hbm.at[:, pl.ds(start, 512)], a_far.at[k], ar_sem.at[0], dp_of(0, 0, 1))
        load_a.wait()
        load_labels.wait()

    with jax.named_scope("relay1"):
        w_take(0, 3, 2, UP, X)
        w_take(0, 1, 3, DOWN, X)
        w_take(0, 3, 3, X)
        w_take(0, 1, 2, X)
        w_take(1, 0, 0, UP, DOWN)
        w_take(1, 0, 1, UP, DOWN)
    with jax.named_scope("relay2"):
        logits_of(0, 0)
        w_take(0, 3, 0, UP)
        w_take(0, 1, 1, DOWN)
        w_take(0, 3, 1)
        w_take(0, 1, 0)
        w_take(1, 0, 2)
        w_take(1, 0, 3)
    with jax.named_scope("relay3"):
        w_take(0, 2, 2, X)
        w_take(0, 2, 3, X)
        logits_of(1, 0)
        logits_of(0, 3)
        logits_of(0, 1)
    with jax.named_scope("relay4"):
        w_take(1, 3, 0, UP)
        w_take(1, 1, 1, DOWN)
        w_take(1, 3, 1)
        w_take(1, 1, 0)
    with jax.named_scope("relay5"):
        for q in (2, 3):
            w_take(1, 3, q)
            w_take(1, 1, q)
        w_take(0, 2, 0)
        w_take(0, 2, 1)
        logits_of(0, 2)
        logits_of(1, 3)
        logits_of(1, 1)
    with jax.named_scope("relay6"):
        for q in range(4):
            w_take(1, 2, q)
        logits_of(1, 2)

    with jax.named_scope("softmax"):
        classes = lax.broadcasted_iota(jnp.int32, (128, width), 1)
        loss_lanes = jnp.zeros((1, 128), F32)
        for t in range(tok // 128):
            lab = jnp.broadcast_to(labels_ref[t : t + 1, :], (128, 128)).T
            lab = jnp.concatenate([lab] * (width // 128), axis=1)
            logits = acc[t * 128 : (t + 1) * 128, :]
            top = jnp.max(logits, axis=1, keepdims=True)
            exps = jnp.exp(logits - top)
            denom = jnp.sum(exps, axis=1, keepdims=True)
            onehot = (lab == classes).astype(F32)
            picked = jnp.sum(logits * onehot, axis=1, keepdims=True)
            probs = exps / denom
            slopes[0, t * 128 : (t + 1) * 128, :] = ((probs - onehot) / tokens).astype(BF16)
            half = slopes.at[0, pl.ds(t * 128, 128), :]
            send(3, half, slopes.at[1, pl.ds(t * 128, 128), :], sr_sem.at[0], dp_of(0, 0, 1))
            term = top + jnp.log(denom) - picked
            loss_lanes += jnp.sum(jnp.broadcast_to(term, (128, 128)), axis=0, keepdims=True)

    pl.semaphore_wait(mid1, 2)
    pl.semaphore_signal(mid2, inc=1, device_id={"layer": away}, device_id_type=MESH)

    def outer(left, right):
        return lax.dot_general(
            left, right, (((0,), (0,)), ((), ())), preferred_element_type=F32
        )

    def near_tokens(k, carry):
        cols = pl.multiple_of(k * chip + c * 384, 128)
        part[k] = outer(a_v[:, pl.ds(cols, 512)], slopes[0])
        return carry

    def at(dx, dy):
        return ((x + dx) % 2) * 4 + (y + dy) % 4

    ahead = ((1, 2), (0, 2), (1, 1), (1, 3))

    def tokens_of(dx, dy):
        k = at(dx, dy)
        if (dx, dy) not in ahead:
            near_tokens(k, 0)
        part[k] += outer(a_far[k], slopes[1])

    with jax.named_scope("own_tokens"):
        for who in ahead:
            near_tokens(at(*who), 0)
    with jax.named_scope("partner"):
        arrived(a_far, ar_sem.at[0])
        arrived(slopes.at[1], sr_sem.at[0])

    def block_rows(q):
        return pl.ds(pl.multiple_of(c * 64 + starts[q], 32), sizes[q])

    def partial(dx, dy, q):
        return part[at(dx, dy), block_rows(q), :]

    def ship(i, value, dest):
        top = jnp.maximum(jnp.max(jnp.abs(value), axis=0, keepdims=True), 1e-30)
        held = pl.ds(0, value.shape[0])
        sbuf[i, held, :] = jnp.round(value * (32767.0 / top)).astype(jnp.int32).astype(jnp.int16)
        sscale[i] = top * (1.0 / 32767.0)
        send(4, sbuf.at[i, held, :], rbuf.at[i, held, :], mr_sem.at[i], dp_of(*dest))
        send(5, sscale.at[i], rscale.at[i], mr_sem.at[i], dp_of(*dest))

    def got(i, q):
        held = pl.ds(0, sizes[q])
        arrived(rscale.at[pl.ds(0, sizes[q] // 2 + 1)], mr_sem.at[i])
        return rbuf[i, held, :].astype(jnp.int32).astype(F32) * rscale[i]

    def x_first(dy, q):
        return dy * 2 + q

    def x_last(q):
        return 8 + q - 2

    def base(side):
        return 10 if side == UP else 19

    def two(side, kind):
        return base(side) + kind

    def one(side, kind, q):
        return base(side) + 3 + kind * 2 + q % 2

    with jax.named_scope("rs_a"):
        tokens_of(1, 2)
        ship(two(UP, 1), partial(1, 2, 2), UP)
        ship(two(DOWN, 1), partial(1, 2, 3), DOWN)
        for q in (0, 1):
            ship(x_first(2, q), partial(1, 2, q), X)
        tokens_of(0, 2)
        ship(two(UP, 0), partial(0, 2, 2), UP)
        ship(two(DOWN, 0), partial(0, 2, 3), DOWN)
    with jax.named_scope("rs_b"):
        tokens_of(1, 1)
        ship(x_first(1, 1), partial(1, 1, 1), X)
        ship(one(UP, 1, 3), partial(1, 1, 3), UP)
        tokens_of(1, 3)
        ship(x_first(3, 0), partial(1, 3, 0), X)
        ship(one(DOWN, 1, 2), partial(1, 3, 2), DOWN)
        tokens_of(0, 1)
        ship(one(UP, 0, 3), partial(0, 1, 3), UP)
        tokens_of(0, 3)
        ship(one(DOWN, 0, 2), partial(0, 3, 2), DOWN)
        ship(x_first(1, 0), partial(1, 1, 0), X)
        ship(x_first(3, 1), partial(1, 3, 1), X)
        tokens_of(1, 0)
        for q in (0, 1):
            ship(x_first(0, q), partial(1, 0, q), X)
        tokens_of(0, 0)
    def up_and_down(kind):
        ship(one(UP, kind, 2), partial(kind, 1, 2) + got(two(UP, kind), 2), UP)
        ship(one(DOWN, kind, 3), partial(kind, 3, 3) + got(two(DOWN, kind), 3), DOWN)

    with jax.named_scope("rs_c1"):
        up_and_down(1)
    with jax.named_scope("rs_d"):
        ship(two(UP, 2), partial(0, 2, 0) + got(x_first(2, 0), 0), UP)
        ship(two(DOWN, 2), partial(0, 2, 1) + got(x_first(2, 1), 1), DOWN)
    with jax.named_scope("rs_c0"):
        up_and_down(0)
    with jax.named_scope("rs_e"):
        ship(one(UP, 2, 1), partial(0, 1, 1) + got(x_first(1, 1), 1), UP)
        ship(one(DOWN, 2, 0), partial(0, 3, 0) + got(x_first(3, 0), 0), DOWN)
    with jax.named_scope("rs_f"):
        pl.semaphore_wait(mid2, 1)
        for q in (3, 2):
            ship(x_last(q), partial(1, 0, q) + got(one(UP, 1, q), q) + got(one(DOWN, 1, q), q), X)
    with jax.named_scope("rs_g"):
        ship(one(UP, 2, 0), partial(0, 1, 0) + got(x_first(1, 0), 0) + got(two(UP, 2), 0), UP)
        ship(one(DOWN, 2, 1), partial(0, 3, 1) + got(x_first(3, 1), 1) + got(two(DOWN, 2), 1), DOWN)

    def finish(q, total, carry):
        for g in range(sizes[q] // 8):
            for j in range(4):
                v = total[g * 8 : (g + 1) * 8, j * 128 : (j + 1) * 128]
                grad_v[pl.ds((starts[q] + g * 8) * 4 + j, 8, stride=4), :] = v
                carry = carry + v * v
        return carry

    square = jnp.zeros((8, 128), F32)
    with jax.named_scope("fin_a"):
        for q in (3, 2):
            total = partial(0, 0, q) + got(one(UP, 0, q), q) + got(one(DOWN, 0, q), q)
            part[at(0, 0), block_rows(q), :] = total
        for q, side in ((1, UP), (0, DOWN)):
            total = partial(0, 0, q) + got(x_first(0, q), q) + got(one(side, 2, q), q)
            part[at(0, 0), block_rows(q), :] = total
    with jax.named_scope("fin_b"):
        for q in (3, 2):
            square = finish(q, partial(0, 0, q) + got(x_last(q), q), square)
    with jax.named_scope("fin_c"):
        for q, side in ((0, UP), (1, DOWN)):
            square = finish(q, partial(0, 0, q) + got(one(side, 2, q), q), square)
        tile = jnp.concatenate([jnp.sum(square, axis=0, keepdims=True), loss_lanes], axis=1)
        store = pltpu.make_async_copy(grad_v, grad_ref, ld_sem.at[3])
        store.start()

    def spread(slots, here, index, peers, stage):
        slots[index] = here
        for who in peers:
            pltpu.make_async_remote_copy(
                src_ref=slots.at[index], dst_ref=slots.at[index], send_sem=sent_sem.at[6 + stage],
                recv_sem=red_sem.at[stage], device_id=who, device_id_type=MESH,
            ).start()
        if stage == 0:
            moved = 7 * rows
            all_sent(0, wbuf.at[pl.ds(0, moved), :])
            all_sent(1, wbuf.at[pl.ds(0, 8 * rows), :])
            all_sent(2, a_far)
            all_sent(3, slopes.at[0])
            all_sent(4, wbuf.at[pl.ds(0, moved), :])
            all_sent(5, sscale)
        some = slots.at[pl.ds(0, len(peers))]
        arrived(some, red_sem.at[stage])
        all_sent(6 + stage, some)
        return jnp.sum(slots[...], axis=0)

    m = y * 2 + c
    n = x * 8 + lay
    with jax.named_scope("red1"):
        tile = spread(
            slots1, tile, m, [{"dp": x * 8 + (m + k) % 8} for k in range(1, 8)], 0
        )
    with jax.named_scope("red2"):
        others = [(n + k) % 16 for k in range(1, 16)]
        sums = spread(
            slots2, tile, n, [{"dp": o // 8 * 8 + m, "layer": o % 8} for o in others], 1
        )
    with jax.named_scope("end1"):
        store.wait()
    square = jnp.broadcast_to(jnp.sum(sums[:, 0:128], axis=1, keepdims=True), (1, 128))
    factor_ref[...] = jnp.minimum(1.0, 0.25 / jnp.sqrt(square + 1e-12))
    loss_ref[...] = sums[:, 128:256] / (tokens * 8)


def shards(activations, labels, weights, first_moment, second_moment):
    tok = activations.shape[0]
    depth = activations.shape[2]
    rows, _, width = weights.shape
    tokens = tok * lax.axis_size("dp")
    dma = pltpu.SemaphoreType.DMA
    vmem = pltpu.VMEM
    lines = rows * width // 128
    anywhere = pl.BlockSpec(memory_space=pltpu.MemorySpace.HBM)
    inside = pl.BlockSpec(memory_space=pltpu.VMEM)

    def body(*refs):
        kernel(tokens, *refs)

    grad, factor, loss = pl.pallas_call(
        body,
        out_shape=(
            jax.ShapeDtypeStruct((lines, 128), F32),
            jax.ShapeDtypeStruct((1, 128), F32),
            jax.ShapeDtypeStruct((1, 128), F32),
        ),
        in_specs=[anywhere, anywhere, anywhere],
        out_specs=(anywhere, inside, inside),
        scratch_shapes=[
            vmem((tok, depth), BF16),
            vmem((tok // 128, 128), jnp.int32),
            vmem((lines, 128), F32),
            vmem((lines, 128), F32),
            vmem((depth, width), BF16),
            vmem((8, tok, 512), BF16),
            vmem((2, tok, width), BF16),
            vmem((tok, width), F32),
            vmem((8, 512, width), F32),
            vmem((28, 128, width), jnp.int16),
            vmem((28, 128, width), jnp.int16),
            vmem((28, 1, width), F32),
            vmem((65, 1, width), F32),
            vmem((8, 1, 256), F32),
            vmem((16, 1, 256), F32),
            dma((4,)),
            dma((8,)),
            dma((8, 4)),
            dma((8,)),
            dma((1,)),
            dma((1,)),
            dma((28,)),
            dma((2,)),
            pltpu.SemaphoreType.REGULAR,
            pltpu.SemaphoreType.REGULAR,
        ],
        compiler_params=pltpu.CompilerParams(
            collective_id=0, has_side_effects=True, vmem_limit_bytes=48 << 20
        ),
        name="probe_step",
    )(
        *(
            pltpu.with_memory_space_constraint(v, pltpu.MemorySpace.HBM)
            for v in (
                activations.reshape(tok, depth),
                labels.reshape(tok // 128, 128),
                weights.reshape(lines, 128),
            )
        )
    )
    held = [v.reshape(lines, 128) for v in (weights, first_moment, second_moment)]
    grad, weights, first_moment, second_moment = lax.optimization_barrier((grad, *held))
    clipped = factor * grad
    new_first = 0.9 * first_moment + 0.1 * clipped
    new_second = 0.999 * second_moment + 0.001 * clipped * clipped
    new_weights = weights - 0.001 * (new_first / (1.0 - 0.9**STEP)) / (
        jnp.sqrt(new_second / (1.0 - 0.999**STEP)) + 1e-08
    )
    outs = (v.reshape(rows, 1, width) for v in (new_weights, new_first, new_second))
    return (*outs, loss[0, 0])


def solution(mesh):
    rows = P("dp", "layer", None)
    return jax.shard_map(
        shards,
        mesh=mesh,
        in_specs=(rows, P("dp"), rows, rows, rows),
        out_specs=(rows, rows, rows, P()),
        check_vma=False,
    )
```

```python
import jax
import jax.numpy as jnp
from jax import lax
from jax.experimental import pallas as pl
from jax.experimental.pallas import tpu as pltpu
from jax.sharding import PartitionSpec as P

STEP = 10
BF16 = jnp.bfloat16
F32 = jnp.float32
MESH = pl.DeviceIdType.MESH


def kernel(
    tokens,
    a_hbm,
    labels_hbm,
    w_hbm,
    grad_ref,
    factor_ref,
    loss_ref,
    a_v,
    labels_ref,
    w32,
    grad_v,
    wbuf,
    a_far,
    slopes,
    acc,
    part,
    sbuf,
    rbuf,
    sscale,
    rscale,
    slots1,
    slots2,
    ld_sem,
    sent_sem,
    wr_sem,
    dr_sem,
    ar_sem,
    sr_sem,
    mr_sem,
    red_sem,
    mid1,
    mid2,
    mid3,
):
    tok = a_v.shape[0]
    width = wbuf.shape[1]
    rows = wbuf.shape[0] // 16
    starts, sizes = (0, 96, 192, 320), (96, 96, 128, 128)
    w_starts, w_sizes = (0, 128, 256, 352), (128, 128, 96, 96)
    chip = 2 * rows
    d = lax.axis_index("dp")
    lay = lax.axis_index("layer")
    x = d // 8
    y = (d // 2) % 4
    c = d % 2

    def dp_of(dx, dy, dc=0):
        return ((x + dx) % 2) * 8 + ((y + dy) % 4) * 2 + (c + dc) % 2

    load_a = pltpu.make_async_copy(a_hbm, a_v, ld_sem.at[0])
    load_w = pltpu.make_async_copy(w_hbm, w32, ld_sem.at[1])
    load_labels = pltpu.make_async_copy(labels_hbm, labels_ref, ld_sem.at[2])
    load_w.start()
    load_a.start()
    load_labels.start()

    away = (lay + 4) % 8
    z_next, z_last = (lay // 4 * 4 + (lay + k) % 4 for k in (1, 3))
    near = [
        {"dp": dp_of(1, 0)},
        {"dp": dp_of(1, 0), "layer": away},
        {"dp": dp_of(0, 1)},
        {"dp": dp_of(0, 3)},
        {"dp": dp_of(0, 0, 1)},
        {"layer": z_next},
        {"layer": z_last},
    ]
    barrier = pltpu.get_barrier_semaphore()
    for who in near:
        pl.semaphore_signal(barrier, inc=1, device_id=who, device_id_type=MESH)

    with jax.named_scope("start"):
        load_w.wait()
        own = pl.multiple_of(d * rows, 64)

        def convert(g, carry):
            for j in range(4):
                v = w32[pl.ds(g * 64 + j, 16, stride=4), :]
                wbuf[pl.ds(pl.multiple_of(own + g * 16, 16), 16), j * 128 : (j + 1) * 128] = v.astype(BF16)
            return carry

        lax.fori_loop(0, rows // 16, convert, 0)
        with jax.named_scope("barrier"):
            pl.semaphore_wait(barrier, len(near))


    def copy_of(src, dst, ssem, rsem, dp):
        return pltpu.make_async_remote_copy(
            src_ref=src, dst_ref=dst, send_sem=ssem, recv_sem=rsem,
            device_id={"dp": dp}, device_id_type=MESH,
        )

    def send(family, src, dst, rsem, dp):
        copy_of(src, dst, sent_sem.at[family], rsem, dp).start()

    def all_sent(family, like):
        copy_of(like, like, sent_sem.at[family], sent_sem.at[family], dp_of(0, 0, 1)).wait_send()

    def arrived(ref, rsem):
        copy_of(ref, ref, sent_sem.at[0], rsem, dp_of(0, 0, 1)).wait_recv()

    def w_rows(dx, dy, dc, q):
        start = pl.multiple_of(dp_of(dx, dy, dc) * rows + w_starts[q], 32)
        return wbuf.at[pl.ds(start, w_sizes[q]), :]

    def w_send(dx, dy, q, *targets):
        ref = w_rows(dx, dy, 0, q)
        for tx, ty in targets:
            k = ((dx - tx) % 2) * 4 + (dy - ty) % 4
            send(0, ref, ref, wr_sem.at[k, q], dp_of(tx, ty))

    def w_pass(dx, dy, q):
        ref = w_rows(dx, dy, 0, q)
        k = dx * 4 + dy
        send(1, ref, ref, dr_sem.at[k], dp_of(0, 0, 1))

    def w_take(dx, dy, q, *targets):
        arrived(w_rows(dx, dy, 0, q), wr_sem.at[dx * 4 + dy, q])
        w_send(dx, dy, q, *targets)
        w_pass(dx, dy, q)

    def chip_cols(dx, dy):
        return pl.multiple_of((((x + dx) % 2) * 4 + (y + dy) % 4) * chip, 128)

    acc[...] = jnp.zeros_like(acc)

    def logits_of(dx, dy):
        cols = chip_cols(dx, dy)
        start = pl.multiple_of(dp_of(dx, dy, 1) * rows, 32)
        arrived(wbuf.at[pl.ds(start, rows), :], dr_sem.at[dx * 4 + dy])

        def step(n, carry):
            lanes = pl.ds(pl.multiple_of(n * 256, 256), 256)
            acc[:, lanes] += jnp.dot(
                a_v[:, pl.ds(cols, chip)], wbuf[pl.ds(cols, chip), lanes],
                preferred_element_type=F32,
            )
            return carry

        lax.fori_loop(0, width // 256, step, 0)

    X, UP, DOWN = (1, 0), (0, 1), (0, 3)
    with jax.named_scope("own"):
        for dest, q in (
            (X, 0), (UP, 2), (DOWN, 3), (X, 1), (UP, 3), (DOWN, 2),
            (X, 2), (UP, 0), (DOWN, 1), (X, 3), (UP, 1), (DOWN, 0),
        ):
            w_send(0, 0, q, dest)
        for q in range(4):
            w_pass(0, 0, q)
        for k in range(8):
            start = pl.multiple_of(k * chip + (1 - c) * 384, 128)
            send(2, a_hbm.at[:, pl.ds(start, 512)], a_far.at[k], ar_sem.at[0], dp_of(0, 0, 1))
        load_a.wait()
        load_labels.wait()

    with jax.named_scope("relay1"):
        w_take(0, 3, 2, UP, X)
        w_take(0, 1, 3, DOWN, X)
        w_take(0, 3, 3, X)
        w_take(0, 1, 2, X)
        w_take(1, 0, 0, UP, DOWN)
        w_take(1, 0, 1, UP, DOWN)
    with jax.named_scope("relay2"):
        logits_of(0, 0)
        w_take(0, 3, 0, UP)
        w_take(0, 1, 1, DOWN)
        w_take(0, 3, 1)
        w_take(0, 1, 0)
        w_take(1, 0, 2)
        w_take(1, 0, 3)
    with jax.named_scope("relay3"):
        w_take(0, 2, 2, X)
        w_take(0, 2, 3, X)
        logits_of(1, 0)
        logits_of(0, 3)
        logits_of(0, 1)
    with jax.named_scope("relay4"):
        w_take(1, 3, 0, UP)
        w_take(1, 1, 1, DOWN)
        w_take(1, 3, 1)
        w_take(1, 1, 0)
    with jax.named_scope("relay5"):
        for q in (2, 3):
            w_take(1, 3, q)
            w_take(1, 1, q)
        w_take(0, 2, 0)
        w_take(0, 2, 1)
        logits_of(0, 2)
        logits_of(1, 3)
        logits_of(1, 1)
    with jax.named_scope("relay6"):
        for q in range(4):
            w_take(1, 2, q)
        logits_of(1, 2)

    with jax.named_scope("softmax"):
        classes = lax.broadcasted_iota(jnp.int32, (128, width), 1)
        loss_lanes = jnp.zeros((1, 128), F32)
        for t in range(tok // 128):
            lab = jnp.broadcast_to(labels_ref[t : t + 1, :], (128, 128)).T
            lab = jnp.concatenate([lab] * (width // 128), axis=1)
            logits = acc[t * 128 : (t + 1) * 128, :]
            top = jnp.max(logits, axis=1, keepdims=True)
            exps = jnp.exp(logits - top)
            denom = jnp.sum(exps, axis=1, keepdims=True)
            onehot = (lab == classes).astype(F32)
            picked = jnp.sum(logits * onehot, axis=1, keepdims=True)
            probs = exps / denom
            slopes[0, t * 128 : (t + 1) * 128, :] = ((probs - onehot) / tokens).astype(BF16)
            half = slopes.at[0, pl.ds(t * 128, 128), :]
            send(3, half, slopes.at[1, pl.ds(t * 128, 128), :], sr_sem.at[0], dp_of(0, 0, 1))
            term = top + jnp.log(denom) - picked
            loss_lanes += jnp.sum(jnp.broadcast_to(term, (128, 128)), axis=0, keepdims=True)

    for who in near[-2:]:
        pl.semaphore_signal(mid1, inc=1, device_id=who, device_id_type=MESH)

    def outer(left, right):
        return lax.dot_general(
            left, right, (((0,), (0,)), ((), ())), preferred_element_type=F32
        )

    def near_tokens(k, carry):
        cols = pl.multiple_of(k * chip + c * 384, 128)
        part[k] = outer(a_v[:, pl.ds(cols, 512)], slopes[0])
        return carry

    def at(dx, dy):
        return ((x + dx) % 2) * 4 + (y + dy) % 4

    ahead = ((1, 2), (0, 2), (1, 1), (1, 3))

    def tokens_of(dx, dy):
        k = at(dx, dy)
        if (dx, dy) not in ahead:
            near_tokens(k, 0)
        part[k] += outer(a_far[k], slopes[1])

    with jax.named_scope("own_tokens"):
        for who in ahead:
            near_tokens(at(*who), 0)
    with jax.named_scope("partner"):
        arrived(a_far, ar_sem.at[0])
        arrived(slopes.at[1], sr_sem.at[0])

    def block_rows(q):
        return pl.ds(pl.multiple_of(c * 64 + starts[q], 32), sizes[q])

    def partial(dx, dy, q):
        return part[at(dx, dy), block_rows(q), :]

    def ship(i, value, dest):
        top = jnp.maximum(jnp.max(jnp.abs(value), axis=0, keepdims=True), 1e-30)
        held = pl.ds(0, value.shape[0])
        sbuf[i, held, :] = jnp.round(value * (32767.0 / top)).astype(jnp.int32).astype(jnp.int16)
        sscale[i] = top * (1.0 / 32767.0)
        send(4, sbuf.at[i, held, :], rbuf.at[i, held, :], mr_sem.at[i], dp_of(*dest))
        send(5, sscale.at[i], rscale.at[i], mr_sem.at[i], dp_of(*dest))

    def got(i, q):
        held = pl.ds(0, sizes[q])
        arrived(rscale.at[pl.ds(0, sizes[q] // 2 + 1)], mr_sem.at[i])
        return rbuf[i, held, :].astype(jnp.int32).astype(F32) * rscale[i]

    def x_first(dy, q):
        return dy * 2 + q

    def x_last(q):
        return 8 + q - 2

    def base(side):
        return 10 if side == UP else 19

    def two(side, kind):
        return base(side) + kind

    def one(side, kind, q):
        return base(side) + 3 + kind * 2 + q % 2

    with jax.named_scope("rs_a"):
        tokens_of(1, 2)
        ship(two(UP, 1), partial(1, 2, 2), UP)
        ship(two(DOWN, 1), partial(1, 2, 3), DOWN)
        for q in (0, 1):
            ship(x_first(2, q), partial(1, 2, q), X)
        tokens_of(0, 2)
        ship(two(UP, 0), partial(0, 2, 2), UP)
        ship(two(DOWN, 0), partial(0, 2, 3), DOWN)
    with jax.named_scope("rs_b"):
        tokens_of(1, 1)
        ship(x_first(1, 1), partial(1, 1, 1), X)
        ship(one(UP, 1, 3), partial(1, 1, 3), UP)
        tokens_of(1, 3)
        ship(x_first(3, 0), partial(1, 3, 0), X)
        ship(one(DOWN, 1, 2), partial(1, 3, 2), DOWN)
        tokens_of(0, 1)
        ship(one(UP, 0, 3), partial(0, 1, 3), UP)
        tokens_of(0, 3)
        ship(one(DOWN, 0, 2), partial(0, 3, 2), DOWN)
        ship(x_first(1, 0), partial(1, 1, 0), X)
        ship(x_first(3, 1), partial(1, 3, 1), X)
        tokens_of(1, 0)
        for q in (0, 1):
            ship(x_first(0, q), partial(1, 0, q), X)
        tokens_of(0, 0)
    def up_and_down(kind):
        ship(one(UP, kind, 2), partial(kind, 1, 2) + got(two(UP, kind), 2), UP)
        ship(one(DOWN, kind, 3), partial(kind, 3, 3) + got(two(DOWN, kind), 3), DOWN)

    with jax.named_scope("rs_c1"):
        up_and_down(1)
    pl.semaphore_wait(mid1, 2)
    for who in near[-2:]:
        pl.semaphore_signal(mid3, inc=1, device_id=who, device_id_type=MESH)
    with jax.named_scope("rs_d"):
        ship(two(UP, 2), partial(0, 2, 0) + got(x_first(2, 0), 0), UP)
        ship(two(DOWN, 2), partial(0, 2, 1) + got(x_first(2, 1), 1), DOWN)
    with jax.named_scope("rs_c0"):
        up_and_down(0)
    with jax.named_scope("rs_e"):
        ship(one(UP, 2, 1), partial(0, 1, 1) + got(x_first(1, 1), 1), UP)
        ship(one(DOWN, 2, 0), partial(0, 3, 0) + got(x_first(3, 0), 0), DOWN)
    with jax.named_scope("rs_f"):
        pl.semaphore_wait(mid3, 2)
        pl.semaphore_signal(mid2, inc=1, device_id={"layer": away}, device_id_type=MESH)
        for q in (3, 2):
            ship(x_last(q), partial(1, 0, q) + got(one(UP, 1, q), q) + got(one(DOWN, 1, q), q), X)
    with jax.named_scope("rs_g"):
        ship(one(UP, 2, 0), partial(0, 1, 0) + got(x_first(1, 0), 0) + got(two(UP, 2), 0), UP)
        ship(one(DOWN, 2, 1), partial(0, 3, 1) + got(x_first(3, 1), 1) + got(two(DOWN, 2), 1), DOWN)

    def finish(q, total, carry):
        for g in range(sizes[q] // 8):
            for j in range(4):
                v = total[g * 8 : (g + 1) * 8, j * 128 : (j + 1) * 128]
                grad_v[pl.ds((starts[q] + g * 8) * 4 + j, 8, stride=4), :] = v
                carry = carry + v * v
        return carry

    square = jnp.zeros((8, 128), F32)
    with jax.named_scope("fin_a"):
        for q in (3, 2):
            total = partial(0, 0, q) + got(one(UP, 0, q), q) + got(one(DOWN, 0, q), q)
            part[at(0, 0), block_rows(q), :] = total
        for q, side in ((1, UP), (0, DOWN)):
            total = partial(0, 0, q) + got(x_first(0, q), q) + got(one(side, 2, q), q)
            part[at(0, 0), block_rows(q), :] = total
    pl.semaphore_wait(mid2, 1)
    with jax.named_scope("fin_b"):
        for q in (3, 2):
            square = finish(q, partial(0, 0, q) + got(x_last(q), q), square)
    with jax.named_scope("fin_c"):
        for q, side in ((0, UP), (1, DOWN)):
            square = finish(q, partial(0, 0, q) + got(one(side, 2, q), q), square)
        tile = jnp.concatenate([jnp.sum(square, axis=0, keepdims=True), loss_lanes], axis=1)
        store = pltpu.make_async_copy(grad_v, grad_ref, ld_sem.at[3])
        store.start()

    def spread(slots, here, index, peers, stage):
        slots[index] = here
        for who in peers:
            pltpu.make_async_remote_copy(
                src_ref=slots.at[index], dst_ref=slots.at[index], send_sem=sent_sem.at[6 + stage],
                recv_sem=red_sem.at[stage], device_id=who, device_id_type=MESH,
            ).start()
        if stage == 0:
            moved = 7 * rows
            all_sent(0, wbuf.at[pl.ds(0, moved), :])
            all_sent(1, wbuf.at[pl.ds(0, 8 * rows), :])
            all_sent(2, a_far)
            all_sent(3, slopes.at[0])
            all_sent(4, wbuf.at[pl.ds(0, moved), :])
            all_sent(5, sscale)
        some = slots.at[pl.ds(0, len(peers))]
        arrived(some, red_sem.at[stage])
        all_sent(6 + stage, some)
        return jnp.sum(slots[...], axis=0)

    with jax.named_scope("red1"):
        tile = spread(slots1, tile, c, [{"dp": dp_of(0, 0, 1)}], 0)
        total = jnp.sum(tile[:, 0:128], axis=1, keepdims=True)
        lower_lanes = lax.broadcasted_iota(jnp.int32, (1, 128), 1) < 64
        tile = jnp.where(lower_lanes, jnp.broadcast_to(total, (1, 128)), tile[:, 128:256])
    chips = [(i, j, k) for i in range(2) for j in range(4) for k in range(8) if i + j + k]
    chips.sort(key=lambda o: -((0, 1, 2, 1)[o[1]] + (0, 1, 2, 1)[o[2] % 4] + (0, 1, 2, 1)[o[2] // 4 * 2 + o[0]]))
    with jax.named_scope("red2"):
        index = (x * 4 + y) * 8 + lay
        sums = spread(
            slots2, tile, index,
            [{"dp": dp_of(i, j), "layer": ((lay // 4 + k // 4) % 2) * 4 + (lay + k) % 4} for i, j, k in chips], 1
        )
    with jax.named_scope("end1"):
        store.wait()
    square = jnp.broadcast_to(sums[:, 0:1], (1, 128))
    factor_ref[...] = jnp.minimum(1.0, 0.25 / jnp.sqrt(square + 1e-12))
    loss_ref[...] = jnp.broadcast_to(sums[:, 127:128], (1, 128)) / (tokens * 8)


def shards(activations, labels, weights, first_moment, second_moment):
    tok = activations.shape[0]
    depth = activations.shape[2]
    rows, _, width = weights.shape
    tokens = tok * lax.axis_size("dp")
    dma = pltpu.SemaphoreType.DMA
    vmem = pltpu.VMEM
    lines = rows * width // 128
    anywhere = pl.BlockSpec(memory_space=pltpu.MemorySpace.HBM)
    inside = pl.BlockSpec(memory_space=pltpu.VMEM)

    def body(*refs):
        kernel(tokens, *refs)

    grad, factor, loss = pl.pallas_call(
        body,
        out_shape=(
            jax.ShapeDtypeStruct((lines, 128), F32),
            jax.ShapeDtypeStruct((1, 128), F32),
            jax.ShapeDtypeStruct((1, 128), F32),
        ),
        in_specs=[anywhere, anywhere, anywhere],
        out_specs=(anywhere, inside, inside),
        scratch_shapes=[
            vmem((tok, depth), BF16),
            vmem((tok // 128, 128), jnp.int32),
            vmem((lines, 128), F32),
            vmem((lines, 128), F32),
            vmem((depth, width), BF16),
            vmem((8, tok, 512), BF16),
            vmem((2, tok, width), BF16),
            vmem((tok, width), F32),
            vmem((8, 512, width), F32),
            vmem((28, 128, width), jnp.int16),
            vmem((28, 128, width), jnp.int16),
            vmem((28, 1, width), F32),
            vmem((65, 1, width), F32),
            vmem((2, 1, 256), F32),
            vmem((64, 1, 128), F32),
            dma((4,)),
            dma((8,)),
            dma((8, 4)),
            dma((8,)),
            dma((1,)),
            dma((1,)),
            dma((28,)),
            dma((2,)),
            pltpu.SemaphoreType.REGULAR,
            pltpu.SemaphoreType.REGULAR,
            pltpu.SemaphoreType.REGULAR,
        ],
        compiler_params=pltpu.CompilerParams(
            collective_id=0, has_side_effects=True, vmem_limit_bytes=48 << 20
        ),
        name="probe_step",
    )(
        *(
            pltpu.with_memory_space_constraint(v, pltpu.MemorySpace.HBM)
            for v in (
                activations.reshape(tok, depth),
                labels.reshape(tok // 128, 128),
                weights.reshape(lines, 128),
            )
        )
    )
    held = [v.reshape(lines, 128) for v in (weights, first_moment, second_moment)]
    grad, weights, first_moment, second_moment = lax.optimization_barrier((grad, *held))
    clipped = factor * grad
    new_first = 0.9 * first_moment + 0.1 * clipped
    new_second = 0.999 * second_moment + 0.001 * clipped * clipped
    new_weights = weights - 0.001 * (new_first / (1.0 - 0.9**STEP)) / (
        jnp.sqrt(new_second / (1.0 - 0.999**STEP)) + 1e-08
    )
    outs = (v.reshape(rows, 1, width) for v in (new_weights, new_first, new_second))
    return (*outs, loss[0, 0])


def solution(mesh):
    rows = P("dp", "layer", None)
    return jax.shard_map(
        shards,
        mesh=mesh,
        in_specs=(rows, P("dp"), rows, rows, rows),
        out_specs=(rows, rows, rows, P()),
        check_vma=False,
    )
```

```python
import jax
import jax.numpy as jnp
from jax import lax
from jax.experimental import pallas as pl
from jax.experimental.pallas import tpu as pltpu
from jax.sharding import PartitionSpec as P

STEP = 10
BF16 = jnp.bfloat16
F32 = jnp.float32
MESH = pl.DeviceIdType.MESH


def kernel(
    tokens,
    a_hbm,
    labels_hbm,
    w_hbm,
    grad_ref,
    factor_ref,
    loss_ref,
    a_v,
    labels_ref,
    w32,
    grad_v,
    wbuf,
    a_far,
    slopes,
    acc,
    part,
    sbuf,
    rbuf,
    sscale,
    rscale,
    slots1,
    slots2,
    ld_sem,
    sent_sem,
    wr_sem,
    dr_sem,
    ar_sem,
    sr_sem,
    mr_sem,
    red_sem,
    mid1,
    mid2,
    mid3,
):
    tok = a_v.shape[0]
    width = wbuf.shape[1]
    rows = wbuf.shape[0] // 16
    starts, sizes = (0, 96, 192, 320), (96, 96, 128, 128)
    w_starts, w_sizes = (0, 128, 256, 352), (128, 128, 96, 96)
    chip = 2 * rows
    d = lax.axis_index("dp")
    lay = lax.axis_index("layer")
    x = d // 8
    y = (d // 2) % 4
    c = d % 2

    def dp_of(dx, dy, dc=0):
        return ((x + dx) % 2) * 8 + ((y + dy) % 4) * 2 + (c + dc) % 2

    load_a = pltpu.make_async_copy(a_hbm, a_v, ld_sem.at[0])
    load_w = pltpu.make_async_copy(w_hbm, w32, ld_sem.at[1])
    load_labels = pltpu.make_async_copy(labels_hbm, labels_ref, ld_sem.at[2])
    load_w.start()
    load_a.start()
    load_labels.start()

    away = (lay + 4) % 8
    z_next, z_last = (lay // 4 * 4 + (lay + k) % 4 for k in (1, 3))
    near = [
        {"dp": dp_of(1, 0)},
        {"dp": dp_of(1, 0), "layer": away},
        {"dp": dp_of(0, 1)},
        {"dp": dp_of(0, 3)},
        {"dp": dp_of(0, 0, 1)},
        {"layer": z_next},
        {"layer": z_last},
    ]
    barrier = pltpu.get_barrier_semaphore()
    for who in near:
        pl.semaphore_signal(barrier, inc=1, device_id=who, device_id_type=MESH)

    with jax.named_scope("start"):
        load_w.wait()
        own = pl.multiple_of(d * rows, 64)

        def convert(g, carry):
            for j in range(4):
                v = w32[pl.ds(g * 64 + j, 16, stride=4), :]
                wbuf[pl.ds(pl.multiple_of(own + g * 16, 16), 16), j * 128 : (j + 1) * 128] = v.astype(BF16)
            return carry

        lax.fori_loop(0, rows // 16, convert, 0)
        with jax.named_scope("barrier"):
            pl.semaphore_wait(barrier, len(near))


    def copy_of(src, dst, ssem, rsem, dp):
        return pltpu.make_async_remote_copy(
            src_ref=src, dst_ref=dst, send_sem=ssem, recv_sem=rsem,
            device_id={"dp": dp}, device_id_type=MESH,
        )

    def send(family, src, dst, rsem, dp):
        copy_of(src, dst, sent_sem.at[family], rsem, dp).start()

    def all_sent(family, like):
        copy_of(like, like, sent_sem.at[family], sent_sem.at[family], dp_of(0, 0, 1)).wait_send()

    def arrived(ref, rsem):
        copy_of(ref, ref, sent_sem.at[0], rsem, dp_of(0, 0, 1)).wait_recv()

    def w_rows(dx, dy, dc, q):
        start = pl.multiple_of(dp_of(dx, dy, dc) * rows + w_starts[q], 32)
        return wbuf.at[pl.ds(start, w_sizes[q]), :]

    def w_send(dx, dy, q, *targets):
        ref = w_rows(dx, dy, 0, q)
        for tx, ty in targets:
            k = ((dx - tx) % 2) * 4 + (dy - ty) % 4
            send(0, ref, ref, wr_sem.at[k, q], dp_of(tx, ty))

    def w_pass(dx, dy, q):
        ref = w_rows(dx, dy, 0, q)
        k = dx * 4 + dy
        send(1, ref, ref, dr_sem.at[k], dp_of(0, 0, 1))

    def w_take(dx, dy, q, *targets):
        arrived(w_rows(dx, dy, 0, q), wr_sem.at[dx * 4 + dy, q])
        w_send(dx, dy, q, *targets)
        w_pass(dx, dy, q)

    def chip_cols(dx, dy):
        return pl.multiple_of((((x + dx) % 2) * 4 + (y + dy) % 4) * chip, 128)

    acc[...] = jnp.zeros_like(acc)

    def logits_of(dx, dy):
        cols = chip_cols(dx, dy)
        start = pl.multiple_of(dp_of(dx, dy, 1) * rows, 32)
        arrived(wbuf.at[pl.ds(start, rows), :], dr_sem.at[dx * 4 + dy])

        def step(n, carry):
            lanes = pl.ds(pl.multiple_of(n * 256, 256), 256)
            acc[:, lanes] += jnp.dot(
                a_v[:, pl.ds(cols, chip)], wbuf[pl.ds(cols, chip), lanes],
                preferred_element_type=F32,
            )
            return carry

        lax.fori_loop(0, width // 256, step, 0)

    X, UP, DOWN = (1, 0), (0, 1), (0, 3)
    with jax.named_scope("own"):
        for dest, q in (
            (X, 0), (UP, 2), (DOWN, 3), (X, 1), (UP, 3), (DOWN, 2),
            (X, 2), (UP, 0), (DOWN, 1), (X, 3), (UP, 1), (DOWN, 0),
        ):
            w_send(0, 0, q, dest)
        for q in range(4):
            w_pass(0, 0, q)
        for k in range(8):
            start = pl.multiple_of(k * chip + (1 - c) * 384, 128)
            send(2, a_hbm.at[:, pl.ds(start, 512)], a_far.at[k], ar_sem.at[0], dp_of(0, 0, 1))
        load_a.wait()
        load_labels.wait()

    with jax.named_scope("relay1"):
        w_take(0, 3, 2, UP, X)
        w_take(0, 1, 3, DOWN, X)
        w_take(0, 3, 3, X)
        w_take(0, 1, 2, X)
        w_take(1, 0, 0, UP, DOWN)
        w_take(1, 0, 1, UP, DOWN)
    with jax.named_scope("relay2"):
        logits_of(0, 0)
        w_take(0, 3, 0, UP)
        w_take(0, 1, 1, DOWN)
        w_take(0, 3, 1)
        w_take(0, 1, 0)
        w_take(1, 0, 2)
        w_take(1, 0, 3)
    with jax.named_scope("relay3"):
        w_take(0, 2, 2, X)
        w_take(0, 2, 3, X)
        logits_of(1, 0)
        logits_of(0, 3)
        logits_of(0, 1)
    with jax.named_scope("relay4"):
        w_take(1, 3, 0, UP)
        w_take(1, 1, 1, DOWN)
        w_take(1, 3, 1)
        w_take(1, 1, 0)
    with jax.named_scope("relay5"):
        for q in (2, 3):
            w_take(1, 3, q)
            w_take(1, 1, q)
        logits_of(1, 3)
        logits_of(1, 1)
        w_take(0, 2, 0)
        w_take(0, 2, 1)
    with jax.named_scope("relay6"):
        for q in (2, 3, 0, 1):
            w_take(1, 2, q)
    with jax.named_scope("relay7"):
        logits_of(0, 2)
        logits_of(1, 2)

    with jax.named_scope("softmax"):
        classes = lax.broadcasted_iota(jnp.int32, (128, width), 1)
        loss_lanes = jnp.zeros((1, 128), F32)
        for t in range(tok // 128):
            lab = jnp.broadcast_to(labels_ref[t : t + 1, :], (128, 128)).T
            lab = jnp.concatenate([lab] * (width // 128), axis=1)
            logits = acc[t * 128 : (t + 1) * 128, :]
            top = jnp.max(logits, axis=1, keepdims=True)
            exps = jnp.exp(logits - top)
            denom = jnp.sum(exps, axis=1, keepdims=True)
            onehot = (lab == classes).astype(F32)
            picked = jnp.sum(logits * onehot, axis=1, keepdims=True)
            probs = exps / denom
            slopes[0, t * 128 : (t + 1) * 128, :] = ((probs - onehot) / tokens).astype(BF16)
            half = slopes.at[0, pl.ds(t * 128, 128), :]
            send(3, half, slopes.at[1, pl.ds(t * 128, 128), :], sr_sem.at[0], dp_of(0, 0, 1))
            term = top + jnp.log(denom) - picked
            loss_lanes += jnp.sum(jnp.broadcast_to(term, (128, 128)), axis=0, keepdims=True)

    for who in near[-2:]:
        pl.semaphore_signal(mid1, inc=1, device_id=who, device_id_type=MESH)

    def outer(left, right):
        return lax.dot_general(
            left, right, (((0,), (0,)), ((), ())), preferred_element_type=F32
        )

    def near_tokens(k, carry):
        cols = pl.multiple_of(k * chip + c * 384, 128)
        part[k] = outer(a_v[:, pl.ds(cols, 512)], slopes[0])
        return carry

    def at(dx, dy):
        return ((x + dx) % 2) * 4 + (y + dy) % 4

    ahead = ((1, 2), (0, 2), (1, 1), (1, 3))

    def tokens_of(dx, dy):
        k = at(dx, dy)
        if (dx, dy) not in ahead:
            near_tokens(k, 0)
        part[k] += outer(a_far[k], slopes[1])

    with jax.named_scope("own_tokens"):
        for who in ahead:
            near_tokens(at(*who), 0)
    with jax.named_scope("partner"):
        arrived(a_far, ar_sem.at[0])
        arrived(slopes.at[1], sr_sem.at[0])

    def block_rows(q):
        return pl.ds(pl.multiple_of(c * 64 + starts[q], 32), sizes[q])

    def partial(dx, dy, q):
        return part[at(dx, dy), block_rows(q), :]

    def ship(i, value, dest):
        top = jnp.maximum(jnp.max(jnp.abs(value), axis=0, keepdims=True), 1e-30)
        held = pl.ds(0, value.shape[0])
        sbuf[i, held, :] = jnp.round(value * (32767.0 / top)).astype(jnp.int32).astype(jnp.int16)
        sscale[i] = top * (1.0 / 32767.0)
        send(4, sbuf.at[i, held, :], rbuf.at[i, held, :], mr_sem.at[i], dp_of(*dest))
        send(5, sscale.at[i], rscale.at[i], mr_sem.at[i], dp_of(*dest))

    def got(i, q):
        held = pl.ds(0, sizes[q])
        arrived(rscale.at[pl.ds(0, sizes[q] // 2 + 1)], mr_sem.at[i])
        return rbuf[i, held, :].astype(jnp.int32).astype(F32) * rscale[i]

    def x_first(dy, q):
        return dy * 2 + q

    def x_last(q):
        return 8 + q - 2

    def base(side):
        return 10 if side == UP else 19

    def two(side, kind):
        return base(side) + kind

    def one(side, kind, q):
        return base(side) + 3 + kind * 2 + q % 2

    with jax.named_scope("rs_a"):
        tokens_of(1, 2)
        ship(two(UP, 1), partial(1, 2, 2), UP)
        ship(two(DOWN, 1), partial(1, 2, 3), DOWN)
        for q in (0, 1):
            ship(x_first(2, q), partial(1, 2, q), X)
        tokens_of(0, 2)
        ship(two(UP, 0), partial(0, 2, 2), UP)
        ship(two(DOWN, 0), partial(0, 2, 3), DOWN)
    with jax.named_scope("rs_b"):
        tokens_of(1, 1)
        ship(x_first(1, 1), partial(1, 1, 1), X)
        ship(one(UP, 1, 3), partial(1, 1, 3), UP)
        tokens_of(1, 3)
        ship(x_first(3, 0), partial(1, 3, 0), X)
        ship(one(DOWN, 1, 2), partial(1, 3, 2), DOWN)
        tokens_of(0, 1)
        ship(one(UP, 0, 3), partial(0, 1, 3), UP)
        tokens_of(0, 3)
        ship(one(DOWN, 0, 2), partial(0, 3, 2), DOWN)
        ship(x_first(1, 0), partial(1, 1, 0), X)
        ship(x_first(3, 1), partial(1, 3, 1), X)
        tokens_of(1, 0)
        for q in (0, 1):
            ship(x_first(0, q), partial(1, 0, q), X)
        tokens_of(0, 0)
    def up_and_down(kind):
        ship(one(UP, kind, 2), partial(kind, 1, 2) + got(two(UP, kind), 2), UP)
        ship(one(DOWN, kind, 3), partial(kind, 3, 3) + got(two(DOWN, kind), 3), DOWN)

    with jax.named_scope("rs_c1"):
        up_and_down(1)
    pl.semaphore_wait(mid1, 2)
    for who in near[-2:]:
        pl.semaphore_signal(mid3, inc=1, device_id=who, device_id_type=MESH)
    with jax.named_scope("rs_d"):
        ship(two(UP, 2), partial(0, 2, 0) + got(x_first(2, 0), 0), UP)
        ship(two(DOWN, 2), partial(0, 2, 1) + got(x_first(2, 1), 1), DOWN)
    with jax.named_scope("rs_c0"):
        up_and_down(0)
    with jax.named_scope("rs_e"):
        ship(one(UP, 2, 1), partial(0, 1, 1) + got(x_first(1, 1), 1), UP)
        ship(one(DOWN, 2, 0), partial(0, 3, 0) + got(x_first(3, 0), 0), DOWN)
    with jax.named_scope("rs_f"):
        pl.semaphore_wait(mid3, 2)
        pl.semaphore_signal(mid2, inc=1, device_id={"layer": away}, device_id_type=MESH)
        for q in (3, 2):
            ship(x_last(q), partial(1, 0, q) + got(one(UP, 1, q), q) + got(one(DOWN, 1, q), q), X)
    with jax.named_scope("rs_g"):
        ship(one(UP, 2, 0), partial(0, 1, 0) + got(x_first(1, 0), 0) + got(two(UP, 2), 0), UP)
        ship(one(DOWN, 2, 1), partial(0, 3, 1) + got(x_first(3, 1), 1) + got(two(DOWN, 2), 1), DOWN)

    def finish(q, total, carry):
        for g in range(sizes[q] // 8):
            for j in range(4):
                v = total[g * 8 : (g + 1) * 8, j * 128 : (j + 1) * 128]
                grad_v[pl.ds((starts[q] + g * 8) * 4 + j, 8, stride=4), :] = v
                carry = carry + v * v
        return carry

    square = jnp.zeros((8, 128), F32)
    with jax.named_scope("fin_a"):
        for q in (3, 2):
            total = partial(0, 0, q) + got(one(UP, 0, q), q) + got(one(DOWN, 0, q), q)
            part[at(0, 0), block_rows(q), :] = total
        for q, side in ((1, UP), (0, DOWN)):
            total = partial(0, 0, q) + got(x_first(0, q), q) + got(one(side, 2, q), q)
            part[at(0, 0), block_rows(q), :] = total
    pl.semaphore_wait(mid2, 1)
    with jax.named_scope("fin_b"):
        for q in (3, 2):
            square = finish(q, partial(0, 0, q) + got(x_last(q), q), square)
    with jax.named_scope("fin_c"):
        for q, side in ((0, UP), (1, DOWN)):
            square = finish(q, partial(0, 0, q) + got(one(side, 2, q), q), square)
        tile = jnp.concatenate([jnp.sum(square, axis=0, keepdims=True), loss_lanes], axis=1)
        store = pltpu.make_async_copy(grad_v, grad_ref, ld_sem.at[3])
        store.start()

    def spread(slots, here, index, peers, stage):
        slots[index] = here
        for who in peers:
            pltpu.make_async_remote_copy(
                src_ref=slots.at[index], dst_ref=slots.at[index], send_sem=sent_sem.at[6 + stage],
                recv_sem=red_sem.at[stage], device_id=who, device_id_type=MESH,
            ).start()
        if stage == 0:
            moved = 7 * rows
            all_sent(0, wbuf.at[pl.ds(0, moved), :])
            all_sent(1, wbuf.at[pl.ds(0, 8 * rows), :])
            all_sent(2, a_far)
            all_sent(3, slopes.at[0])
            all_sent(4, wbuf.at[pl.ds(0, moved), :])
            all_sent(5, sscale)
        some = slots.at[pl.ds(0, len(peers))]
        arrived(some, red_sem.at[stage])
        all_sent(6 + stage, some)
        return jnp.sum(slots[...], axis=0)

    with jax.named_scope("red1"):
        tile = spread(slots1, tile, c, [{"dp": dp_of(0, 0, 1)}], 0)
        total = jnp.sum(tile[:, 0:128], axis=1, keepdims=True)
        lower_lanes = lax.broadcasted_iota(jnp.int32, (1, 128), 1) < 64
        tile = jnp.where(lower_lanes, jnp.broadcast_to(total, (1, 128)), tile[:, 128:256])
    chips = [(i, j, k) for i in range(2) for j in range(4) for k in range(8) if i + j + k]
    chips.sort(key=lambda o: -((0, 1, 2, 1)[o[1]] + (0, 1, 2, 1)[o[2] % 4] + (0, 1, 2, 1)[o[2] // 4 * 2 + o[0]]))
    with jax.named_scope("red2"):
        index = (x * 4 + y) * 8 + lay
        sums = spread(
            slots2, tile, index,
            [{"dp": dp_of(i, j), "layer": ((lay // 4 + k // 4) % 2) * 4 + (lay + k) % 4} for i, j, k in chips], 1
        )
    with jax.named_scope("end1"):
        store.wait()
    square = jnp.broadcast_to(sums[:, 0:1], (1, 128))
    factor_ref[...] = jnp.minimum(1.0, 0.25 / jnp.sqrt(square + 1e-12))
    loss_ref[...] = jnp.broadcast_to(sums[:, 127:128], (1, 128)) / (tokens * 8)


def shards(activations, labels, weights, first_moment, second_moment):
    tok = activations.shape[0]
    depth = activations.shape[2]
    rows, _, width = weights.shape
    tokens = tok * lax.axis_size("dp")
    dma = pltpu.SemaphoreType.DMA
    vmem = pltpu.VMEM
    lines = rows * width // 128
    anywhere = pl.BlockSpec(memory_space=pltpu.MemorySpace.HBM)
    inside = pl.BlockSpec(memory_space=pltpu.VMEM)

    def body(*refs):
        kernel(tokens, *refs)

    grad, factor, loss = pl.pallas_call(
        body,
        out_shape=(
            jax.ShapeDtypeStruct((lines, 128), F32),
            jax.ShapeDtypeStruct((1, 128), F32),
            jax.ShapeDtypeStruct((1, 128), F32),
        ),
        in_specs=[anywhere, anywhere, anywhere],
        out_specs=(anywhere, inside, inside),
        scratch_shapes=[
            vmem((tok, depth), BF16),
            vmem((tok // 128, 128), jnp.int32),
            vmem((lines, 128), F32),
            vmem((lines, 128), F32),
            vmem((depth, width), BF16),
            vmem((8, tok, 512), BF16),
            vmem((2, tok, width), BF16),
            vmem((tok, width), F32),
            vmem((8, 512, width), F32),
            vmem((28, 128, width), jnp.int16),
            vmem((28, 128, width), jnp.int16),
            vmem((28, 1, width), F32),
            vmem((65, 1, width), F32),
            vmem((2, 1, 256), F32),
            vmem((64, 1, 128), F32),
            dma((4,)),
            dma((8,)),
            dma((8, 4)),
            dma((8,)),
            dma((1,)),
            dma((1,)),
            dma((28,)),
            dma((2,)),
            pltpu.SemaphoreType.REGULAR,
            pltpu.SemaphoreType.REGULAR,
            pltpu.SemaphoreType.REGULAR,
        ],
        compiler_params=pltpu.CompilerParams(
            collective_id=0, has_side_effects=True, vmem_limit_bytes=48 << 20
        ),
        name="probe_step",
    )(
        *(
            pltpu.with_memory_space_constraint(v, pltpu.MemorySpace.HBM)
            for v in (
                activations.reshape(tok, depth),
                labels.reshape(tok // 128, 128),
                weights.reshape(lines, 128),
            )
        )
    )
    held = [v.reshape(lines, 128) for v in (weights, first_moment, second_moment)]
    grad, weights, first_moment, second_moment = lax.optimization_barrier((grad, *held))
    clipped = factor * grad
    new_first = 0.9 * first_moment + 0.1 * clipped
    new_second = 0.999 * second_moment + 0.001 * clipped * clipped
    new_weights = weights - 0.001 * (new_first / (1.0 - 0.9**STEP)) / (
        jnp.sqrt(new_second / (1.0 - 0.999**STEP)) + 1e-08
    )
    outs = (v.reshape(rows, 1, width) for v in (new_weights, new_first, new_second))
    return (*outs, loss[0, 0])


def solution(mesh):
    rows = P("dp", "layer", None)
    return jax.shard_map(
        shards,
        mesh=mesh,
        in_specs=(rows, P("dp"), rows, rows, rows),
        out_specs=(rows, rows, rows, P()),
        check_vma=False,
    )
```

```python
import jax
import jax.numpy as jnp
from jax import lax
from jax.experimental import pallas as pl
from jax.experimental.pallas import tpu as pltpu
from jax.sharding import PartitionSpec as P

STEP = 10
BF16 = jnp.bfloat16
F32 = jnp.float32
MESH = pl.DeviceIdType.MESH


def kernel(
    tokens,
    a_hbm,
    labels_hbm,
    w_hbm,
    grad_ref,
    factor_ref,
    loss_ref,
    a_v,
    labels_ref,
    w32,
    grad_v,
    wbuf,
    a_far,
    slopes,
    acc,
    part,
    sbuf,
    rbuf,
    sscale,
    rscale,
    slots1,
    slots2,
    ld_sem,
    sent_sem,
    wr_sem,
    dr_sem,
    ar_sem,
    sr_sem,
    mr_sem,
    red_sem,
    mid1,
    mid2,
    mid3,
):
    tok = a_v.shape[0]
    width = wbuf.shape[1]
    rows = wbuf.shape[0] // 16
    starts, sizes = (0, 96, 192, 320), (96, 96, 128, 128)
    w_starts, w_sizes = (0, 128, 256, 352), (128, 128, 96, 96)
    chip = 2 * rows
    d = lax.axis_index("dp")
    lay = lax.axis_index("layer")
    x = d // 8
    y = (d // 2) % 4
    c = d % 2

    def dp_of(dx, dy, dc=0):
        return ((x + dx) % 2) * 8 + ((y + dy) % 4) * 2 + (c + dc) % 2

    load_a = pltpu.make_async_copy(a_hbm, a_v, ld_sem.at[0])
    load_w = pltpu.make_async_copy(w_hbm, w32, ld_sem.at[1])
    load_labels = pltpu.make_async_copy(labels_hbm, labels_ref, ld_sem.at[2])
    load_w.start()
    load_a.start()
    load_labels.start()

    away = (lay + 4) % 8
    z_next, z_last = (lay // 4 * 4 + (lay + k) % 4 for k in (1, 3))
    near = [
        {"dp": dp_of(1, 0)},
        {"dp": dp_of(1, 0), "layer": away},
        {"dp": dp_of(0, 1)},
        {"dp": dp_of(0, 3)},
        {"dp": dp_of(0, 0, 1)},
        {"layer": z_next},
        {"layer": z_last},
    ]
    barrier = pltpu.get_barrier_semaphore()
    for who in near:
        pl.semaphore_signal(barrier, inc=1, device_id=who, device_id_type=MESH)

    with jax.named_scope("start"):
        load_w.wait()
        own = pl.multiple_of(d * rows, 64)

        def convert(g, carry):
            for j in range(4):
                v = w32[pl.ds(g * 64 + j, 16, stride=4), :]
                wbuf[pl.ds(pl.multiple_of(own + g * 16, 16), 16), j * 128 : (j + 1) * 128] = v.astype(BF16)
            return carry

        lax.fori_loop(0, rows // 16, convert, 0)
        with jax.named_scope("barrier"):
            pl.semaphore_wait(barrier, len(near))


    def copy_of(src, dst, ssem, rsem, dp):
        return pltpu.make_async_remote_copy(
            src_ref=src, dst_ref=dst, send_sem=ssem, recv_sem=rsem,
            device_id={"dp": dp}, device_id_type=MESH,
        )

    def send(family, src, dst, rsem, dp):
        copy_of(src, dst, sent_sem.at[family], rsem, dp).start()

    def all_sent(family, like):
        copy_of(like, like, sent_sem.at[family], sent_sem.at[family], dp_of(0, 0, 1)).wait_send()

    def arrived(ref, rsem):
        copy_of(ref, ref, sent_sem.at[0], rsem, dp_of(0, 0, 1)).wait_recv()

    def w_rows(dx, dy, dc, q):
        start = pl.multiple_of(dp_of(dx, dy, dc) * rows + w_starts[q], 32)
        return wbuf.at[pl.ds(start, w_sizes[q]), :]

    def w_send(dx, dy, q, *targets):
        ref = w_rows(dx, dy, 0, q)
        for tx, ty in targets:
            k = ((dx - tx) % 2) * 4 + (dy - ty) % 4
            send(0, ref, ref, wr_sem.at[k, q], dp_of(tx, ty))

    def w_pass(dx, dy, q):
        ref = w_rows(dx, dy, 0, q)
        k = dx * 4 + dy
        send(1, ref, ref, dr_sem.at[k], dp_of(0, 0, 1))

    def w_take(dx, dy, q, *targets):
        arrived(w_rows(dx, dy, 0, q), wr_sem.at[dx * 4 + dy, q])
        w_send(dx, dy, q, *targets)
        w_pass(dx, dy, q)

    def chip_cols(dx, dy):
        return pl.multiple_of((((x + dx) % 2) * 4 + (y + dy) % 4) * chip, 128)

    acc[...] = jnp.zeros_like(acc)

    def logits_of(dx, dy):
        cols = chip_cols(dx, dy)
        start = pl.multiple_of(dp_of(dx, dy, 1) * rows, 32)
        arrived(wbuf.at[pl.ds(start, rows), :], dr_sem.at[dx * 4 + dy])

        def step(n, carry):
            lanes = pl.ds(pl.multiple_of(n * 256, 256), 256)
            acc[:, lanes] += jnp.dot(
                a_v[:, pl.ds(cols, chip)], wbuf[pl.ds(cols, chip), lanes],
                preferred_element_type=F32,
            )
            return carry

        lax.fori_loop(0, width // 256, step, 0)

    X, UP, DOWN = (1, 0), (0, 1), (0, 3)
    with jax.named_scope("own"):
        for dest, q in (
            (X, 0), (UP, 2), (DOWN, 3), (X, 1), (UP, 3), (DOWN, 2),
            (X, 2), (UP, 0), (DOWN, 1), (X, 3), (UP, 1), (DOWN, 0),
        ):
            w_send(0, 0, q, dest)
        for q in range(4):
            w_pass(0, 0, q)
        for k in range(8):
            start = pl.multiple_of(k * chip + (1 - c) * 384, 128)
            send(2, a_hbm.at[:, pl.ds(start, 512)], a_far.at[k], ar_sem.at[0], dp_of(0, 0, 1))
        load_a.wait()
        load_labels.wait()

    with jax.named_scope("relay1"):
        w_take(0, 3, 2, UP, X)
        w_take(0, 1, 3, DOWN, X)
        w_take(0, 3, 3, X)
        w_take(0, 1, 2, X)
        w_take(1, 0, 0, UP, DOWN)
        w_take(1, 0, 1, UP, DOWN)
    with jax.named_scope("relay2"):
        logits_of(0, 0)
        w_take(0, 3, 0, UP)
        w_take(0, 1, 1, DOWN)
        w_take(0, 3, 1)
        w_take(0, 1, 0)
        w_take(1, 0, 2)
        w_take(1, 0, 3)
    with jax.named_scope("relay3"):
        w_take(0, 2, 2, X)
        w_take(0, 2, 3, X)
        logits_of(1, 0)
        logits_of(0, 3)
        logits_of(0, 1)
    with jax.named_scope("relay4"):
        w_take(1, 3, 0, UP)
        w_take(1, 1, 1, DOWN)
        w_take(1, 3, 1)
        w_take(1, 1, 0)
    with jax.named_scope("relay5"):
        for q in (2, 3):
            w_take(1, 3, q)
            w_take(1, 1, q)
        logits_of(1, 3)
        logits_of(1, 1)
        w_take(0, 2, 0)
        w_take(0, 2, 1)
    with jax.named_scope("relay6"):
        for q in (2, 3, 0, 1):
            w_take(1, 2, q)
    with jax.named_scope("relay7"):
        logits_of(0, 2)
        logits_of(1, 2)

    with jax.named_scope("softmax"):
        classes = lax.broadcasted_iota(jnp.int32, (128, width), 1)
        loss_lanes = jnp.zeros((1, 128), F32)
        for t in range(tok // 128):
            lab = jnp.broadcast_to(labels_ref[t : t + 1, :], (128, 128)).T
            lab = jnp.concatenate([lab] * (width // 128), axis=1)
            logits = acc[t * 128 : (t + 1) * 128, :]
            top = jnp.max(logits, axis=1, keepdims=True)
            exps = jnp.exp(logits - top)
            denom = jnp.sum(exps, axis=1, keepdims=True)
            onehot = (lab == classes).astype(F32)
            picked = jnp.sum(logits * onehot, axis=1, keepdims=True)
            probs = exps / denom
            slopes[0, t * 128 : (t + 1) * 128, :] = ((probs - onehot) / tokens).astype(BF16)
            term = top + jnp.log(denom) - picked
            loss_lanes += jnp.sum(jnp.broadcast_to(term, (128, 128)), axis=0, keepdims=True)

    send(3, slopes.at[0], slopes.at[1], sr_sem.at[0], dp_of(0, 0, 1))
    for who in near[-2:]:
        pl.semaphore_signal(mid1, inc=1, device_id=who, device_id_type=MESH)

    def outer(left, right):
        return lax.dot_general(
            left, right, (((0,), (0,)), ((), ())), preferred_element_type=F32
        )

    def near_tokens(k, carry):
        cols = pl.multiple_of(k * chip + c * 384, 128)
        part[k] = outer(a_v[:, pl.ds(cols, 512)], slopes[0])
        return carry

    def at(dx, dy):
        return ((x + dx) % 2) * 4 + (y + dy) % 4

    ahead = ((1, 2), (0, 2), (1, 1), (1, 3))

    def tokens_of(dx, dy):
        k = at(dx, dy)
        if (dx, dy) not in ahead:
            near_tokens(k, 0)
        part[k] += outer(a_far[k], slopes[1])

    with jax.named_scope("own_tokens"):
        for who in ahead:
            near_tokens(at(*who), 0)
    with jax.named_scope("partner"):
        arrived(a_far, ar_sem.at[0])
        arrived(slopes.at[1], sr_sem.at[0])

    def block_rows(q):
        return pl.ds(pl.multiple_of(c * 64 + starts[q], 32), sizes[q])

    def partial(dx, dy, q):
        return part[at(dx, dy), block_rows(q), :]

    def ship(i, value, dest):
        top = jnp.maximum(jnp.max(jnp.abs(value), axis=0, keepdims=True), 1e-30)
        held = pl.ds(0, value.shape[0])
        sbuf[i, held, :] = jnp.round(value * (32767.0 / top)).astype(jnp.int32).astype(jnp.int16)
        sscale[i] = top * (1.0 / 32767.0)
        send(4, sbuf.at[i, held, :], rbuf.at[i, held, :], mr_sem.at[i], dp_of(*dest))
        send(5, sscale.at[i], rscale.at[i], mr_sem.at[i], dp_of(*dest))

    def got(i, q):
        held = pl.ds(0, sizes[q])
        arrived(rscale.at[pl.ds(0, sizes[q] // 2 + 1)], mr_sem.at[i])
        return rbuf[i, held, :].astype(jnp.int32).astype(F32) * rscale[i]

    def x_first(dy, q):
        return dy * 2 + q

    def x_last(q):
        return 8 + q - 2

    def base(side):
        return 10 if side == UP else 19

    def two(side, kind):
        return base(side) + kind

    def one(side, kind, q):
        return base(side) + 3 + kind * 2 + q % 2

    with jax.named_scope("rs_a"):
        tokens_of(1, 2)
        ship(two(UP, 1), partial(1, 2, 2), UP)
        ship(two(DOWN, 1), partial(1, 2, 3), DOWN)
        for q in (0, 1):
            ship(x_first(2, q), partial(1, 2, q), X)
        tokens_of(0, 2)
        ship(two(UP, 0), partial(0, 2, 2), UP)
        ship(two(DOWN, 0), partial(0, 2, 3), DOWN)
    with jax.named_scope("rs_b"):
        tokens_of(1, 1)
        ship(x_first(1, 1), partial(1, 1, 1), X)
        ship(one(UP, 1, 3), partial(1, 1, 3), UP)
        tokens_of(1, 3)
        ship(x_first(3, 0), partial(1, 3, 0), X)
        ship(one(DOWN, 1, 2), partial(1, 3, 2), DOWN)
        tokens_of(0, 1)
        ship(one(UP, 0, 3), partial(0, 1, 3), UP)
        tokens_of(0, 3)
        ship(one(DOWN, 0, 2), partial(0, 3, 2), DOWN)
        ship(x_first(1, 0), partial(1, 1, 0), X)
        ship(x_first(3, 1), partial(1, 3, 1), X)
        tokens_of(1, 0)
        for q in (0, 1):
            ship(x_first(0, q), partial(1, 0, q), X)
        tokens_of(0, 0)
    def up_and_down(kind):
        ship(one(UP, kind, 2), partial(kind, 1, 2) + got(two(UP, kind), 2), UP)
        ship(one(DOWN, kind, 3), partial(kind, 3, 3) + got(two(DOWN, kind), 3), DOWN)

    with jax.named_scope("rs_c1"):
        up_and_down(1)
    pl.semaphore_wait(mid1, 2)
    for who in near[-2:]:
        pl.semaphore_signal(mid3, inc=1, device_id=who, device_id_type=MESH)
    with jax.named_scope("rs_d"):
        ship(two(UP, 2), partial(0, 2, 0) + got(x_first(2, 0), 0), UP)
        ship(two(DOWN, 2), partial(0, 2, 1) + got(x_first(2, 1), 1), DOWN)
    with jax.named_scope("rs_c0"):
        up_and_down(0)
    with jax.named_scope("rs_e"):
        ship(one(UP, 2, 1), partial(0, 1, 1) + got(x_first(1, 1), 1), UP)
        ship(one(DOWN, 2, 0), partial(0, 3, 0) + got(x_first(3, 0), 0), DOWN)
    with jax.named_scope("rs_f"):
        pl.semaphore_wait(mid3, 2)
        pl.semaphore_signal(mid2, inc=1, device_id={"layer": away}, device_id_type=MESH)
        for q in (3, 2):
            ship(x_last(q), partial(1, 0, q) + got(one(UP, 1, q), q) + got(one(DOWN, 1, q), q), X)
    with jax.named_scope("rs_g"):
        ship(one(UP, 2, 0), partial(0, 1, 0) + got(x_first(1, 0), 0) + got(two(UP, 2), 0), UP)
        ship(one(DOWN, 2, 1), partial(0, 3, 1) + got(x_first(3, 1), 1) + got(two(DOWN, 2), 1), DOWN)

    def finish(q, total, carry):
        for g in range(sizes[q] // 8):
            for j in range(4):
                v = total[g * 8 : (g + 1) * 8, j * 128 : (j + 1) * 128]
                grad_v[pl.ds((starts[q] + g * 8) * 4 + j, 8, stride=4), :] = v
                carry = carry + v * v
        return carry

    square = jnp.zeros((8, 128), F32)
    with jax.named_scope("fin_a"):
        for q in (3, 2):
            total = partial(0, 0, q) + got(one(UP, 0, q), q) + got(one(DOWN, 0, q), q)
            part[at(0, 0), block_rows(q), :] = total
        for q, side in ((1, UP), (0, DOWN)):
            total = partial(0, 0, q) + got(x_first(0, q), q) + got(one(side, 2, q), q)
            part[at(0, 0), block_rows(q), :] = total
    pl.semaphore_wait(mid2, 1)
    with jax.named_scope("fin_b"):
        for q in (3, 2):
            square = finish(q, partial(0, 0, q) + got(x_last(q), q), square)
    with jax.named_scope("fin_c"):
        for q, side in ((0, UP), (1, DOWN)):
            square = finish(q, partial(0, 0, q) + got(one(side, 2, q), q), square)
        tile = jnp.concatenate([jnp.sum(square, axis=0, keepdims=True), loss_lanes], axis=1)
        store = pltpu.make_async_copy(grad_v, grad_ref, ld_sem.at[3])
        store.start()

    def spread(slots, here, index, peers, stage):
        slots[index] = here
        for who in peers:
            pltpu.make_async_remote_copy(
                src_ref=slots.at[index], dst_ref=slots.at[index], send_sem=sent_sem.at[6 + stage],
                recv_sem=red_sem.at[stage], device_id=who, device_id_type=MESH,
            ).start()
        if stage == 0:
            moved = 7 * rows
            all_sent(0, wbuf.at[pl.ds(0, moved), :])
            all_sent(1, wbuf.at[pl.ds(0, 8 * rows), :])
            all_sent(2, a_far)
            all_sent(3, slopes.at[0])
            all_sent(4, wbuf.at[pl.ds(0, moved), :])
            all_sent(5, sscale)
        some = slots.at[pl.ds(0, len(peers))]
        arrived(some, red_sem.at[stage])
        all_sent(6 + stage, some)
        return jnp.sum(slots[...], axis=0)

    with jax.named_scope("red1"):
        tile = spread(slots1, tile, c, [{"dp": dp_of(0, 0, 1)}], 0)
        total = jnp.sum(tile[:, 0:128], axis=1, keepdims=True)
        lower_lanes = lax.broadcasted_iota(jnp.int32, (1, 128), 1) < 64
        tile = jnp.where(lower_lanes, jnp.broadcast_to(total, (1, 128)), tile[:, 128:256])
    chips = [(i, j, k) for i in range(2) for j in range(4) for k in range(8) if i + j + k]
    chips.sort(key=lambda o: -((0, 1, 2, 1)[o[1]] + (0, 1, 2, 1)[o[2] % 4] + (0, 1, 2, 1)[o[2] // 4 * 2 + o[0]]))
    with jax.named_scope("red2"):
        index = (x * 4 + y) * 8 + lay
        sums = spread(
            slots2, tile, index,
            [{"dp": dp_of(i, j), "layer": ((lay // 4 + k // 4) % 2) * 4 + (lay + k) % 4} for i, j, k in chips], 1
        )
    with jax.named_scope("end1"):
        store.wait()
    square = jnp.broadcast_to(sums[:, 0:1], (1, 128))
    factor_ref[...] = jnp.minimum(1.0, 0.25 / jnp.sqrt(square + 1e-12))
    loss_ref[...] = jnp.broadcast_to(sums[:, 127:128], (1, 128)) / (tokens * 8)


def shards(activations, labels, weights, first_moment, second_moment):
    tok = activations.shape[0]
    depth = activations.shape[2]
    rows, _, width = weights.shape
    tokens = tok * lax.axis_size("dp")
    dma = pltpu.SemaphoreType.DMA
    vmem = pltpu.VMEM
    lines = rows * width // 128
    anywhere = pl.BlockSpec(memory_space=pltpu.MemorySpace.HBM)
    inside = pl.BlockSpec(memory_space=pltpu.VMEM)

    def body(*refs):
        kernel(tokens, *refs)

    grad, factor, loss = pl.pallas_call(
        body,
        out_shape=(
            jax.ShapeDtypeStruct((lines, 128), F32),
            jax.ShapeDtypeStruct((1, 128), F32),
            jax.ShapeDtypeStruct((1, 128), F32),
        ),
        in_specs=[anywhere, anywhere, anywhere],
        out_specs=(anywhere, inside, inside),
        scratch_shapes=[
            vmem((tok, depth), BF16),
            vmem((tok // 128, 128), jnp.int32),
            vmem((lines, 128), F32),
            vmem((lines, 128), F32),
            vmem((depth, width), BF16),
            vmem((8, tok, 512), BF16),
            vmem((2, tok, width), BF16),
            vmem((tok, width), F32),
            vmem((8, 512, width), F32),
            vmem((28, 128, width), jnp.int16),
            vmem((28, 128, width), jnp.int16),
            vmem((28, 1, width), F32),
            vmem((65, 1, width), F32),
            vmem((2, 1, 256), F32),
            vmem((64, 1, 128), F32),
            dma((4,)),
            dma((8,)),
            dma((8, 4)),
            dma((8,)),
            dma((1,)),
            dma((1,)),
            dma((28,)),
            dma((2,)),
            pltpu.SemaphoreType.REGULAR,
            pltpu.SemaphoreType.REGULAR,
            pltpu.SemaphoreType.REGULAR,
        ],
        compiler_params=pltpu.CompilerParams(
            collective_id=0, has_side_effects=True, vmem_limit_bytes=48 << 20
        ),
        name="probe_step",
    )(
        *(
            pltpu.with_memory_space_constraint(v, pltpu.MemorySpace.HBM)
            for v in (
                activations.reshape(tok, depth),
                labels.reshape(tok // 128, 128),
                weights.reshape(lines, 128),
            )
        )
    )
    held = [v.reshape(lines, 128) for v in (weights, first_moment, second_moment)]
    grad, weights, first_moment, second_moment = lax.optimization_barrier((grad, *held))
    clipped = factor * grad
    new_first = 0.9 * first_moment + 0.1 * clipped
    new_second = 0.999 * second_moment + 0.001 * clipped * clipped
    new_weights = weights - 0.001 * (new_first / (1.0 - 0.9**STEP)) / (
        jnp.sqrt(new_second / (1.0 - 0.999**STEP)) + 1e-08
    )
    outs = (v.reshape(rows, 1, width) for v in (new_weights, new_first, new_second))
    return (*outs, loss[0, 0])


def solution(mesh):
    rows = P("dp", "layer", None)
    return jax.shard_map(
        shards,
        mesh=mesh,
        in_specs=(rows, P("dp"), rows, rows, rows),
        out_specs=(rows, rows, rows, P()),
        check_vma=False,
    )
```
